32 devices in a mesh: w: 4 (over z), h: 8 (over y, x, core).
Axes of the slice: x: 2, y: 2, z: 4, core: 2. Of those that a mesh axis runs over, the one named last changes fastest.
Arguments:
- x: bfloat16 [1, 256, 1024, 128], P(None, 'h', 'w')
- w1: bfloat16 [3, 3, 128, 128], replicated
- gamma: float32 [128], replicated
- beta: float32 [128], replicated
- w2: bfloat16 [3, 3, 128, 128], replicated
- g: bfloat16 [1, 256, 1024, 128], P(None, 'h', 'w')
Outputs:
- output 1: bfloat16 [1, 256, 1024, 128], P(None, 'h', 'w')
- output 2: bfloat16 [1, 256, 1024, 128], P(None, 'h', 'w')
- output 3: float32 [3, 3, 128, 128], replicated
- output 4: float32 [3, 3, 128, 128], replicated
- output 5: float32 [128], replicated
- output 6: float32 [128], replicated
All inputs are finite; a program needn't handle non-finite values.
Results may differ from the reference program's by a relative error of at most 0.00104032.
Values are sent between devices in bfloat16 or wider.
A program may use at most 1 GiB of HBM per device.

```python
import jax
import jax.numpy as jnp
from jax import lax

B = 1
C = 128
GROUPS = 32
TH = 32
TW = 256
HT = 8
WT = 4
HS = HT * TH
WS = WT * TW
DN = ('NHWC', 'HWIO', 'NHWC')


def setup_inputs(seed: int = 0) -> dict:
    ks = jax.random.split(jax.random.PRNGKey(seed), 6)
    rows = jnp.arange(HS)
    cols = jnp.arange(WS)
    xs = (0.5 + 1.5 * rows / HS)[None, :, None, None]
    x = (jax.random.normal(ks[0], (B, HS, WS, C), jnp.float32) * xs).astype(jnp.bfloat16)
    std = (9 * C) ** -0.5
    w1 = (jax.random.normal(ks[1], (3, 3, C, C), jnp.float32) * std).astype(jnp.bfloat16)
    gamma = 1.0 + 0.3 * jax.random.normal(ks[2], (C,), jnp.float32)
    beta = 0.3 * jax.random.normal(ks[3], (C,), jnp.float32)
    w2 = (jax.random.normal(ks[4], (3, 3, C, C), jnp.float32) * std).astype(jnp.bfloat16)
    edge = ((rows % TH == 0) | (rows % TH == TH - 1))[:, None] | ((cols % TW == 0) | (cols % TW == TW - 1))[None, :]
    gs = jnp.where(edge, 3.0, 1.0)[None, :, :, None]
    g = (jax.random.normal(ks[5], (B, HS, WS, C), jnp.float32) * gs).astype(jnp.bfloat16)
    return {'x': x, 'w1': w1, 'gamma': gamma, 'beta': beta, 'w2': w2, 'g': g}


def _conv(u, w):
    return lax.conv_general_dilated(u.astype(jnp.float32), w.astype(jnp.float32), (1, 1), 'SAME', dimension_numbers=DN)


def _conv_t(v, w):
    return _conv(v, jnp.flip(w, (0, 1)).transpose(0, 1, 3, 2))


def _wgrad(u, v):
    up = jnp.pad(u.astype(jnp.float32), ((0, 0), (1, 1), (1, 1), (0, 0)))
    v32 = v.astype(jnp.float32)
    h, w = v.shape[1], v.shape[2]
    return jnp.stack([jnp.stack([jnp.einsum('bhwc,bhwo->co', up[:, a:a + h, b:b + w], v32) for b in range(3)]) for a in range(3)])


def _norm_act(a, gamma, beta):
    nb, h, w, c = a.shape
    ag = a.reshape(nb, h, w, GROUPS, c // GROUPS)
    mean = ag.mean(axis=(1, 2, 4), keepdims=True)
    var = ((ag - mean) ** 2).mean(axis=(1, 2, 4), keepdims=True)
    n = ((ag - mean) * lax.rsqrt(var + 1e-5)).reshape(a.shape) * gamma + beta
    return jax.nn.gelu(n, approximate=True)


def reference(x, w1, gamma, beta, w2, g):
    a = _conv(x, w1).astype(jnp.bfloat16).astype(jnp.float32)
    zf, vjp = jax.vjp(_norm_act, a, gamma, beta)
    z = zf.astype(jnp.bfloat16)
    y = (_conv(z, w2) + x.astype(jnp.float32)).astype(jnp.bfloat16)
    dz = _conv_t(g, w2)
    dw2 = _wgrad(z, g)
    da, dgamma, dbeta = vjp(dz)
    da = da.astype(jnp.bfloat16)
    dx = (_conv_t(da, w1) + g.astype(jnp.float32)).astype(jnp.bfloat16)
    dw1 = _wgrad(x, da)
    return y, dx, dw1, dw2, dgamma, dbeta
```

```python
import functools

import jax
import jax.numpy as jnp
from jax import lax
from jax.experimental import pallas as pl
from jax.experimental.pallas import tpu as pltpu
from jax.sharding import PartitionSpec as P

MESH = pl.DeviceIdType.MESH
GROUPS = 32
EPS = 1e-5
RB, TB, NT, SL = 64, 16, 9, 8
C = 128
BF = jnp.bfloat16
F32 = jnp.float32
GC = 0.7978845608028654
GC2 = GC * 0.044715
DIRS = ((-1, 0), (1, 0), (0, -1), (0, 1), (-1, -1), (-1, 1), (1, -1), (1, 1))
OPP = (1, 0, 3, 2, 7, 6, 5, 4)


def _group_sum(v):
    lane = lax.broadcasted_iota(jnp.int32, v.shape, 1)
    v = v + jnp.where(lane % 2 == 0, pltpu.roll(v, C - 1, 1), pltpu.roll(v, 1, 1))
    return v + jnp.where(lane % 4 < 2, pltpu.roll(v, C - 2, 1), pltpu.roll(v, 2, 1))


def _fold(v):
    return v.reshape(v.shape[0] // SL, SL, C).sum(0)


def _kernel(nh, nw, th, tw, x_hbm, g_hbm, w1_hbm, w2_hbm, gam_ref, bet_ref,
            y_hbm, dx_hbm, dw1_hbm, dw2_hbm, dgam_ref, dbet_ref,
            xv, gv, w1v, w2v, wc1, wt1, wc2, wt2, ucat, gcat, zcat, gt, dat, av, dn, row, yv,
            hr, hc, hk, hrd, hcd, hkd, ec,
            st, sbuf, tt, tbuf, wacc, dwl, rd, rxy, zb, ag,
            ld, hs, hv, ss, sr, rs, rr, ysem):
    w = lax.axis_index('w')
    h = lax.axis_index('h')
    ndev = nh * nw
    me = w * nh + h
    cnt = float(th * nh * tw * nw * (C // GROUPS))

    barrier = pltpu.get_barrier_semaphore()

    @pl.loop(1, ndev)
    def _(k):
        d = lax.rem(me + k, ndev)
        pl.semaphore_signal(barrier, inc=1, device_id=(d // nh, d % nh), device_id_type=MESH)

    loads = [pltpu.make_async_copy(s, d, ld.at[i]) for i, (s, d) in enumerate(
        ((x_hbm, xv), (w1_hbm, w1v), (g_hbm, gv), (w2_hbm, w2v)))]
    for c in loads:
        c.start()

    def neighbour(d):
        dy, dx = DIRS[d]
        hh, ww = h + dy, w + dx
        ok = (hh >= 0) & (hh < nh) & (ww >= 0) & (ww < nw)
        return ok, (ww, hh)

    def halo(t, rows, cols, hrow, hcol, hcor, start):
        for d, (dy, dx) in enumerate(DIRS):
            ok, dev = neighbour(d)
            o = OPP[d]
            r = 0 if dy < 0 else th - 1
            if dx == 0:
                src, dst = rows.at[r], hrow.at[o]
            elif dy == 0:
                src, dst = cols.at[d - 2], hcol.at[o - 2]
            else:
                src, dst = rows.at[r, pl.ds(0 if dx < 0 else tw - TB, TB)], hcor.at[o - 4]
            cp = pltpu.make_async_remote_copy(src, dst, hs.at[t, d], hv.at[t, o], device_id=dev, device_id_type=MESH)
            if start:
                pl.when(ok)(cp.start)
            else:
                back = pltpu.make_async_remote_copy(
                    src, (hrow.at[d] if dx == 0 else hcol.at[d - 2] if dy == 0 else hcor.at[d - 4]),
                    hs.at[t, d], hv.at[t, d], device_id=dev, device_id_type=MESH)

                @pl.when(ok)
                def _():
                    back.wait_send()
                    back.wait_recv()

    def oks():
        return [neighbour(d)[0] for d in range(SL)]

    def cat_row(cat, r):
        for j in range(0, tw, RB):
            for b in range(3):
                cat[r, pl.ds(j, RB), pl.ds(b * C, C)] = row[pl.ds(7 + b + j, RB), :].astype(BF)

    def set_ends(left, right):
        row[7:SL, :] = left
        row[tw + SL:tw + NT, :] = right

    def patch(cat, r, left, right):
        it = lax.broadcasted_iota(jnp.int32, (TB, C), 0)
        a = cat[r, 0:TB, 0:C].astype(F32)
        cat[r, 0:TB, 0:C] = jnp.where(it == 0, left, a).astype(BF)
        b = cat[r, tw - TB:tw, 2 * C:3 * C].astype(F32)
        cat[r, tw - TB:tw, 2 * C:3 * C] = jnp.where(it == 15, right, b).astype(BF)

    def halo_rows(cat, okl, f, hrow, hcol, hcor):
        for e, r in ((0, 0), (1, th + 1)):
            for j in range(0, tw, RB):
                row[pl.ds(SL + j, RB), :] = jnp.where(okl[e], f([b[e, pl.ds(j, RB), :].astype(F32) for b in hrow]), 0.0)
            kl, kr = 2 * e, 2 * e + 1
            cl = f([b[kl].astype(F32) for b in hcor])
            cr = f([b[kr].astype(F32) for b in hcor])
            set_ends(jnp.where(okl[4 + kl], cl[15:TB, :], 0.0), jnp.where(okl[4 + kr], cr[0:1, :], 0.0))
            cat_row(cat, r)

        @pl.loop(0, th // SL)
        def _(k):
            r8 = pl.multiple_of(k * SL, SL)
            lf = jnp.where(okl[2], f([b[0, pl.ds(r8, SL), :].astype(F32) for b in hcol]), 0.0)
            rg = jnp.where(okl[3], f([b[1, pl.ds(r8, SL), :].astype(F32) for b in hcol]), 0.0)
            for i in range(SL):
                patch(cat, r8 + i + 1, lf[i:i + 1, :], rg[i:i + 1, :])

    def build(src, cat, t, vt):
        @pl.loop(0, th)
        def _(r):
            for j in range(0, tw, RB):
                row[pl.ds(SL + j, RB), :] = src[r, pl.ds(j, RB), :].astype(F32)
            ec[t, 0, pl.ds(r, 1), :] = row[SL:NT, :]
            ec[t, 1, pl.ds(r, 1), :] = row[tw + 7:tw + SL, :]
            cat_row(cat, r + 1)
            if vt is not None:
                vt[r + 1] = src[r].T

    def weights(wv, wc, wt):
        for r in range(4):
            for b in range(3):
                for t in range(2):
                    a = r - t
                    sl = (pl.ds((r * 3 + b) * C, C), pl.ds(t * C, C))
                    if 0 <= a < 3:
                        wc[sl] = wv[a * 3 + b]
                        wt[sl] = wv[(2 - a) * 3 + 2 - b].T
                    else:
                        wc[sl] = jnp.zeros((C, C), BF)
                        wt[sl] = jnp.zeros((C, C), BF)

    def conv(cat, wc, lo, hi, carry, fn):
        def step(q, carry):
            lhs = jnp.concatenate([
                jnp.concatenate([cat[4 * q + 2 * p + r] for r in range(4)], axis=1) for p in range(2)], axis=0)
            o = jnp.dot(lhs, wc[...], preferred_element_type=F32)
            return fn(q, o, carry)
        return lax.fori_loop(lo, hi, step, carry)

    def rows_of(o):
        return [o[(i // 2) * tw:(i // 2 + 1) * tw, (i % 2) * C:(i % 2 + 1) * C] for i in range(4)]

    def wgrad(vt, cat, dst):
        zero = jnp.zeros((C, tw), BF)
        vt[0] = zero
        vt[th + 1] = zero
        wacc[...] = jnp.zeros_like(wacc)
        wacc[0:C, :] = jnp.dot(vt[1], cat[0], preferred_element_type=F32)
        wacc[2 * C:3 * C, :] = jnp.dot(vt[th], cat[th + 1], preferred_element_type=F32)

        @pl.loop(0, th // 4)
        def _(q):
            lhs = jnp.concatenate([
                jnp.concatenate([vt[4 * q + s + 2 - a] for a in range(3)], axis=0) for s in range(4)], axis=1)
            rhs = cat[pl.ds(4 * q + 1, 4)].reshape(4 * tw, 3 * C)
            wacc[...] += jnp.dot(lhs, rhs, preferred_element_type=F32)

        for a in range(3):
            for b in range(3):
                dst[pl.ds((a * 3 + b) * C, C), :] = wacc[a * C:(a + 1) * C, b * C:(b + 1) * C].T

    def spread(src, buf, i):
        buf[me] = src[...]

        @pl.loop(1, ndev)
        def _(k):
            d = lax.rem(me + k, ndev)
            pltpu.make_async_remote_copy(src, buf.at[me], ss.at[i], sr.at[i], device_id=(d // nh, d % nh),
                                         device_id_type=MESH).start()

    def gather(buf, i):
        part = buf.at[pl.ds(0, ndev - 1)]
        pltpu.make_async_copy(part, part, sr.at[i]).wait()
        pltpu.make_async_copy(part, part, ss.at[i]).wait()
        s = buf[0]
        for k in range(1, ndev):
            s = s + buf[k]
        return s

    core, q_me = h % 2, h // 2
    half, piece = NT * C // 2, NT * C // SL

    def rcopy(src, dst, i, k, dev):
        return pltpu.make_async_remote_copy(src, dst, rs.at[i, k], rr.at[i, k], device_id=dev, device_id_type=MESH)

    def at(ref, i, start, n):
        return ref.at[i, pl.ds(pl.multiple_of(start, TB), n)]

    def ar_pair(i):
        other = 1 - core
        return rcopy(at(dwl, i, other * half, half), rd.at[i], i, 0, (w, h + 1 - 2 * core))

    def ar_xy(i):
        cps = []
        for k in range(1, 4):
            qo = q_me ^ k
            cps.append(rcopy(at(dwl, i, core * half + qo * piece, piece), rxy.at[i, k - 1], i, k, (w, qo * 2 + core)))
        return cps

    def ar_z(i):
        return [rcopy(zb.at[i, w], zb.at[i, w], i, 3 + k, (lax.rem(w + k, nw), h)) for k in range(1, nw)]

    def ar_z_in(i):
        return [rcopy(zb.at[i, w], zb.at[i, lax.rem(w + nw - k, nw)], i, 3 + k, (w, h)) for k in range(1, nw)]

    def ar_xy2(i):
        mine = at(ag, i, core * half + q_me * piece, piece)
        return [rcopy(mine, mine, i, 6 + k, (w, (q_me ^ k) * 2 + core)) for k in range(1, 4)]

    def ar_xy2_in(i):
        mine = at(ag, i, core * half + q_me * piece, piece)
        return [rcopy(mine, at(ag, i, core * half + (q_me ^ k) * piece, piece), i, 6 + k, (w, h)) for k in range(1, 4)]

    def ar_pair2(i):
        mine = at(ag, i, core * half, half)
        return rcopy(mine, mine, i, 10, (w, h + 1 - 2 * core))

    def ar_pair2_in(i):
        mine = at(ag, i, core * half, half)
        return rcopy(mine, at(ag, i, (1 - core) * half, half), i, 10, (w, h))

    outs = (dw1_hbm, dw2_hbm)

    def out_copy(i, c, k):
        s = pl.ds(pl.multiple_of(c * half, TB), half)
        return pltpu.make_async_copy(ag.at[i, s], outs[i].at[s], ysem.at[2 + 2 * i + k])

    def ar_step(i, n):
        if n == 0:
            ar_pair(i).start()
        elif n == 1:
            ar_pair(i).wait()
            for k in range(4):
                s = pl.ds(pl.multiple_of(core * half + k * piece, TB), piece)
                dwl[i, s, :] = dwl[i, s, :] + rd[i, pl.ds(k * piece, piece), :]
            for c in ar_xy(i):
                c.start()
        elif n == 2:
            for c in ar_xy(i):
                c.wait()
            s = pl.ds(pl.multiple_of(core * half + q_me * piece, TB), piece)
            zb[i, w] = dwl[i, s, :] + rxy[i, 0] + rxy[i, 1] + rxy[i, 2]
            for c in ar_z(i):
                c.start()
        elif n == 3:
            for c in ar_z(i):
                c.wait_send()
            for c in ar_z_in(i):
                c.wait_recv()
            s = zb[i, 0]
            for k in range(1, nw):
                s = s + zb[i, k]
            ag[i, pl.ds(pl.multiple_of(core * half + q_me * piece, TB), piece), :] = s
            for c in ar_xy2(i):
                c.start()
        elif n == 4:
            for c in ar_xy2(i):
                c.wait_send()
            for c in ar_xy2_in(i):
                c.wait_recv()
            ar_pair2(i).start()
            out_copy(i, core, 0).start()
        else:
            ar_pair2(i).wait_send()
            ar_pair2_in(i).wait_recv()
            out_copy(i, 1 - core, 1).start()

    okl = oks()
    loads[0].wait()
    build(xv, ucat, 0, None)
    loads[1].wait()
    weights(w1v, wc1, wt1)
    pl.semaphore_wait(barrier, ndev - 1)
    halo(0, xv, ec.at[0], hr.at[0], hc.at[0], hk.at[0], True)
    loads[2].wait()
    build(gv, gcat, 1, gt)
    halo(1, gv, ec.at[1], hr.at[1], hc.at[1], hk.at[1], True)
    loads[3].wait()
    weights(w2v, wc2, wt2)
    halo(0, xv, ec.at[0], hr.at[0], hc.at[0], hk.at[0], False)
    halo_rows(ucat, okl, lambda v: v[0], [hr.at[0]], [hc.at[0]], [hk.at[0]])

    def fin_a(q, o, carry):
        s1, s2 = carry
        for i, v in enumerate(rows_of(o)):
            vb = v.astype(BF)
            av[4 * q + i] = vb
            vf = vb.astype(F32)
            ec[2, 0, pl.ds(4 * q + i, 1), :] = vf[0:1, :]
            ec[2, 1, pl.ds(4 * q + i, 1), :] = vf[tw - 1:tw, :]
            s1 = s1 + _fold(vf)
            s2 = s2 + _fold(vf * vf)
        return s1, s2

    z8 = jnp.zeros((SL, C), F32)
    s1, s2 = conv(ucat, wc1, 0, th // 4, (z8, z8), fin_a)
    st[0:1, :] = s1.sum(0, keepdims=True)
    st[1:2, :] = s2.sum(0, keepdims=True)
    spread(st, sbuf, 0)
    halo(2, av, ec.at[2], hr.at[2], hc.at[2], hk.at[2], True)

    halo(1, gv, ec.at[1], hr.at[1], hc.at[1], hk.at[1], False)
    halo_rows(gcat, okl, lambda v: v[0], [hr.at[1]], [hc.at[1]], [hk.at[1]])

    def fin_dz(q, o, carry):
        for i, v in enumerate(rows_of(o)):
            dn[4 * q + i] = v
        return carry

    conv(gcat, wt2, 0, th // 4, 0, fin_dz)

    tot = _group_sum(gather(sbuf, 0)) / cnt
    mean = tot[0:1, :]
    rstd = lax.rsqrt(tot[1:2, :] - mean * mean + EPS)
    sh = -mean * rstd
    gam = gam_ref[...]
    bet = bet_ref[...]

    def act(a):
        xh = a * rstd + sh
        n = xh * gam + bet
        n2 = n * n
        p = 0.5 + 0.5 * jnp.tanh(n * (GC + GC2 * n2))
        return xh, n2, p, n * p

    def zrow(r, carry):
        t0, t1 = carry
        for j in range(0, tw, RB):
            s = pl.ds(j, RB)
            xh, n2, p, z = act(av[r, s, :].astype(F32))
            row[pl.ds(SL + j, RB), :] = z
            d = dn[r, s, :] * (p + z * (1.0 - p) * (2.0 * GC + 6.0 * GC2 * n2))
            dn[r, s, :] = d
            if j == 0:
                ec[3, 0, pl.ds(r, 1), :] = d[0:1, :]
            if j + RB == tw:
                ec[3, 1, pl.ds(r, 1), :] = d[63:RB, :]
            t0 = t0 + _fold(d * xh)
            t1 = t1 + _fold(d)
        cat_row(zcat, r + 1)
        return t0, t1

    t0, t1 = lax.fori_loop(0, th, zrow, (z8, z8))
    tt[0:1, :] = t0.sum(0, keepdims=True)
    tt[1:2, :] = t1.sum(0, keepdims=True)
    spread(tt, tbuf, 1)
    halo(3, dn, ec.at[3], hrd, hcd, hkd, True)

    halo(2, av, ec.at[2], hr.at[2], hc.at[2], hk.at[2], False)
    halo_rows(zcat, okl, lambda v: act(v[0])[3], [hr.at[2]], [hc.at[2]], [hk.at[2]])

    wgrad(gt, zcat, dwl.at[1])
    ar_step(1, 0)

    t = gather(tbuf, 1)
    dgam_ref[...] = t[0:1, :]
    dbet_ref[...] = t[1:2, :]
    u = _group_sum(t * gam) / cnt
    k1 = gam * rstd
    k2 = -rstd * rstd * u[0:1, :]
    k3 = -rstd * (u[1:2, :] + sh * u[0:1, :])

    @pl.loop(0, th)
    def _(r):
        for j in range(0, tw, RB):
            s = pl.ds(j, RB)
            v = dn[r, s, :] * k1 + av[r, s, :].astype(F32) * k2 + k3
            row[pl.ds(SL + j, RB), :] = v
        cat_row(gcat, r + 1)
        dat[r + 1] = gcat[r + 1, :, C:2 * C].T

    halo(3, dn, ec.at[3], hrd, hcd, hkd, False)
    halo_rows(gcat, okl, lambda v: v[0] * k1 + v[1] * k2 + k3, [hrd, hr.at[2]], [hcd, hc.at[2]], [hkd, hk.at[2]])
    ar_step(1, 1)

    wgrad(dat, ucat, dwl.at[0])
    ar_step(0, 0)
    ar_step(1, 2)

    def ycopy(k, q):
        s = pl.ds(4 * q, 4)
        return pltpu.make_async_copy(yv.at[k, s], (dx_hbm, y_hbm)[k].at[s], ysem.at[k])

    def fin_dx(q, o, carry):
        for i, v in enumerate(rows_of(o)):
            yv[0, 4 * q + i] = (v + gv[4 * q + i].astype(F32)).astype(BF)
        ycopy(0, q).start()
        return carry

    def fin_y(q, o, carry):
        for i, v in enumerate(rows_of(o)):
            yv[1, 4 * q + i] = (v + xv[4 * q + i].astype(F32)).astype(BF)
        ycopy(1, q).start()
        return carry

    n4 = th // 4
    conv(gcat, wt1, 0, n4 // 2, 0, fin_dx)
    ar_step(0, 1)
    ar_step(1, 3)
    conv(gcat, wt1, n4 // 2, n4, 0, fin_dx)
    ar_step(0, 2)
    ar_step(1, 4)
    conv(zcat, wc2, 0, n4, 0, fin_y)
    ar_step(0, 3)
    ar_step(1, 5)
    ar_step(0, 4)
    pltpu.make_async_copy(yv.at[0], dx_hbm, ysem.at[0]).wait()
    pltpu.make_async_copy(yv.at[1], y_hbm, ysem.at[1]).wait()
    ar_step(0, 5)
    for i in range(2):
        out_copy(i, core, 0).wait()
        out_copy(i, 1 - core, 1).wait()


def solution(mesh):
    nh, nw = mesh.shape['h'], mesh.shape['w']
    tile = P(None, 'h', 'w', None)

    def body(x, w1, gamma, beta, w2, g):
        _, th, tw, c = x.shape
        anys = pl.BlockSpec(memory_space=pl.ANY)
        vm = pl.BlockSpec(memory_space=pltpu.VMEM)
        V = pltpu.VMEM
        D = pltpu.SemaphoreType.DMA
        img = jax.ShapeDtypeStruct((th, tw, c), BF)
        wsh = jax.ShapeDtypeStruct((NT * c, c), F32)
        vec = jax.ShapeDtypeStruct((1, c), F32)
        cat = V((th + 2, tw, 3 * c), BF)
        ndev = nh * nw
        scratch = dict(
            xv=V((th, tw, c), BF), gv=V((th, tw, c), BF), w1v=V((NT, c, c), BF), w2v=V((NT, c, c), BF),
            wc1=V((12 * c, 2 * c), BF), wt1=V((12 * c, 2 * c), BF), wc2=V((12 * c, 2 * c), BF), wt2=V((12 * c, 2 * c), BF),
            ucat=cat, gcat=cat, zcat=cat, gt=V((th + 2, c, tw), BF), dat=V((th + 2, c, tw), BF),
            av=V((th, tw, c), BF), dn=V((th, tw, c), F32), row=V((tw + TB, c), F32), yv=V((2, th, tw, c), BF),
            hr=V((3, 2, tw, c), BF), hc=V((3, 2, th, c), F32), hk=V((3, 4, TB, c), BF),
            hrd=V((2, tw, c), F32), hcd=V((2, th, c), F32), hkd=V((4, TB, c), F32), ec=V((4, 2, th, c), F32),
            st=V((2, c), F32), sbuf=V((ndev, 2, c), F32), tt=V((2, c), F32), tbuf=V((ndev, 2, c), F32),
            wacc=V((3 * c, 3 * c), F32), dwl=V((2, NT * c, c), F32), rd=V((2, NT * c // 2, c), F32),
            rxy=V((2, 3, NT * c // SL, c), F32), zb=V((2, nw, NT * c // SL, c), F32), ag=V((2, NT * c, c), F32),
            ld=D((4,)), hs=D((4, SL)), hv=D((4, SL)), ss=D((2,)), sr=D((2,)), rs=D((2, 11)), rr=D((2, 11)), ysem=D((6,)),
        )
        y, dx, dw1, dw2, dg, db = pl.pallas_call(
            functools.partial(_kernel, nh, nw, th, tw),
            out_shape=(img, img, wsh, wsh, vec, vec),
            in_specs=[anys] * 4 + [vm] * 2,
            out_specs=(anys,) * 4 + (vm,) * 2,
            scratch_shapes=list(scratch.values()),
            compiler_params=pltpu.CompilerParams(collective_id=0, has_side_effects=True, vmem_limit_bytes=62 << 20),
        )(x.reshape(th, tw, c), g.reshape(th, tw, c), w1.reshape(NT, c, c), w2.reshape(NT, c, c),
          gamma.reshape(1, c), beta.reshape(1, c))
        return (y.reshape(x.shape), dx.reshape(x.shape), dw1.reshape(3, 3, c, c), dw2.reshape(3, 3, c, c),
                dg.reshape(c), db.reshape(c))

    return jax.shard_map(body, mesh=mesh, in_specs=(tile, P(), P(), P(), P(), tile),
                         out_specs=(tile, tile, P(), P(), P(), P()), check_vma=False)
```

```python
import functools

import jax
import jax.numpy as jnp
from jax import lax
from jax.experimental import pallas as pl
from jax.experimental.pallas import tpu as pltpu
from jax.sharding import PartitionSpec as P

MESH = pl.DeviceIdType.MESH
GROUPS = 32
EPS = 1e-5
RB, TB, NT, SL = 64, 16, 9, 8
C = 128
BF = jnp.bfloat16
F32 = jnp.float32
GC = 0.7978845608028654
GC2 = GC * 0.044715
DIRS = ((-1, 0), (1, 0), (0, -1), (0, 1), (-1, -1), (-1, 1), (1, -1), (1, 1))
OPP = (1, 0, 3, 2, 7, 6, 5, 4)


def _group_sum(v):
    lane = lax.broadcasted_iota(jnp.int32, v.shape, 1)
    v = v + jnp.where(lane % 2 == 0, pltpu.roll(v, C - 1, 1), pltpu.roll(v, 1, 1))
    return v + jnp.where(lane % 4 < 2, pltpu.roll(v, C - 2, 1), pltpu.roll(v, 2, 1))


def _fold(v):
    return v.reshape(v.shape[0] // SL, SL, C).sum(0)


def _kernel(nh, nw, th, tw, x_hbm, g_hbm, w1v, w2v, gam_ref, bet_ref,
            y_ref, dx_ref, dw1_ref, dw2_ref, dgam_ref, dbet_ref,
            xv, gv, wc1, wt1, wc2, wt2, ucat, gcat, zcat, gt, dat, av, dn, row,
            hr, hc, hk, hrd, hcd, hkd, ec,
            st, sbuf, tt, tbuf, wacc, dwl, rd, rxy, zb,
            ld, hs, hv, ss, sr, rs, rr):
    w = lax.axis_index('w')
    h = lax.axis_index('h')
    ndev = nh * nw
    me = w * nh + h
    cnt = float(th * nh * tw * nw * (C // GROUPS))

    barrier = pltpu.get_barrier_semaphore()

    @pl.loop(1, ndev)
    def _(k):
        d = lax.rem(me + k, ndev)
        pl.semaphore_signal(barrier, inc=1, device_id=(d // nh, d % nh), device_id_type=MESH)

    loads = [pltpu.make_async_copy(s, d, ld.at[i]) for i, (s, d) in enumerate(
        ((x_hbm, xv), (g_hbm, gv)))]
    for c in loads:
        c.start()

    def neighbour(d):
        dy, dx = DIRS[d]
        hh, ww = h + dy, w + dx
        ok = (hh >= 0) & (hh < nh) & (ww >= 0) & (ww < nw)
        return ok, (ww, hh)

    def halo(t, rows, cols, hrow, hcol, hcor, start):
        for d, (dy, dx) in enumerate(DIRS):
            ok, dev = neighbour(d)
            o = OPP[d]
            r = 0 if dy < 0 else th - 1
            if dx == 0:
                src, dst = rows.at[r], hrow.at[o]
            elif dy == 0:
                src, dst = cols.at[d - 2], hcol.at[o - 2]
            else:
                src, dst = rows.at[r, pl.ds(0 if dx < 0 else tw - TB, TB)], hcor.at[o - 4]
            cp = pltpu.make_async_remote_copy(src, dst, hs.at[t, d], hv.at[t, o], device_id=dev, device_id_type=MESH)
            if start:
                pl.when(ok)(cp.start)
            else:
                back = pltpu.make_async_remote_copy(
                    src, (hrow.at[d] if dx == 0 else hcol.at[d - 2] if dy == 0 else hcor.at[d - 4]),
                    hs.at[t, d], hv.at[t, d], device_id=dev, device_id_type=MESH)

                @pl.when(ok)
                def _():
                    back.wait_send()
                    back.wait_recv()

    def oks():
        return [neighbour(d)[0] for d in range(SL)]

    def cat_row(cat, r):
        for j in range(0, tw, RB):
            for b in range(3):
                cat[r, pl.ds(j, RB), pl.ds(b * C, C)] = row[pl.ds(7 + b + j, RB), :].astype(BF)

    def set_ends(left, right):
        row[7:SL, :] = left
        row[tw + SL:tw + NT, :] = right

    def patch(cat, r, left, right):
        it = lax.broadcasted_iota(jnp.int32, (TB, C), 0)
        a = cat[r, 0:TB, 0:C].astype(F32)
        cat[r, 0:TB, 0:C] = jnp.where(it == 0, left, a).astype(BF)
        b = cat[r, tw - TB:tw, 2 * C:3 * C].astype(F32)
        cat[r, tw - TB:tw, 2 * C:3 * C] = jnp.where(it == 15, right, b).astype(BF)

    def halo_rows(cat, okl, f, hrow, hcol, hcor):
        for e, r in ((0, 0), (1, th + 1)):
            for j in range(0, tw, RB):
                row[pl.ds(SL + j, RB), :] = jnp.where(okl[e], f([b[e, pl.ds(j, RB), :].astype(F32) for b in hrow]), 0.0)
            kl, kr = 2 * e, 2 * e + 1
            cl = f([b[kl].astype(F32) for b in hcor])
            cr = f([b[kr].astype(F32) for b in hcor])
            set_ends(jnp.where(okl[4 + kl], cl[15:TB, :], 0.0), jnp.where(okl[4 + kr], cr[0:1, :], 0.0))
            cat_row(cat, r)

        @pl.loop(0, th // SL)
        def _(k):
            r8 = pl.multiple_of(k * SL, SL)
            lf = jnp.where(okl[2], f([b[0, pl.ds(r8, SL), :].astype(F32) for b in hcol]), 0.0)
            rg = jnp.where(okl[3], f([b[1, pl.ds(r8, SL), :].astype(F32) for b in hcol]), 0.0)
            for i in range(SL):
                patch(cat, r8 + i + 1, lf[i:i + 1, :], rg[i:i + 1, :])

    def build(src, cat, t, vt):
        @pl.loop(0, th)
        def _(r):
            for j in range(0, tw, RB):
                row[pl.ds(SL + j, RB), :] = src[r, pl.ds(j, RB), :].astype(F32)
            ec[t, 0, pl.ds(r, 1), :] = row[SL:NT, :]
            ec[t, 1, pl.ds(r, 1), :] = row[tw + 7:tw + SL, :]
            cat_row(cat, r + 1)
            if vt is not None:
                vt[r + 1] = src[r].T

    def weights(wv, wc, wt):
        for r in range(4):
            for b in range(3):
                for t in range(2):
                    a = r - t
                    sl = (pl.ds((r * 3 + b) * C, C), pl.ds(t * C, C))
                    if 0 <= a < 3:
                        wc[sl] = wv[a * 3 + b]
                        wt[sl] = wv[(2 - a) * 3 + 2 - b].T
                    else:
                        wc[sl] = jnp.zeros((C, C), BF)
                        wt[sl] = jnp.zeros((C, C), BF)

    def conv(cat, wc, lo, hi, carry, fn):
        def step(q, carry):
            lhs = jnp.concatenate([
                jnp.concatenate([cat[4 * q + 2 * p + r] for r in range(4)], axis=1) for p in range(2)], axis=0)
            o = jnp.dot(lhs, wc[...], preferred_element_type=F32)
            return fn(q, o, carry)
        return lax.fori_loop(lo, hi, step, carry)

    def rows_of(o):
        return [o[(i // 2) * tw:(i // 2 + 1) * tw, (i % 2) * C:(i % 2 + 1) * C] for i in range(4)]

    def wgrad(vt, cat, dst):
        zero = jnp.zeros((C, tw), BF)
        vt[0] = zero
        vt[th + 1] = zero
        wacc[...] = jnp.zeros_like(wacc)
        wacc[0:C, :] = jnp.dot(vt[1], cat[0], preferred_element_type=F32)
        wacc[2 * C:3 * C, :] = jnp.dot(vt[th], cat[th + 1], preferred_element_type=F32)

        @pl.loop(0, th // 4)
        def _(q):
            lhs = jnp.concatenate([
                jnp.concatenate([vt[4 * q + s + 2 - a] for a in range(3)], axis=0) for s in range(4)], axis=1)
            rhs = cat[pl.ds(4 * q + 1, 4)].reshape(4 * tw, 3 * C)
            wacc[...] += jnp.dot(lhs, rhs, preferred_element_type=F32)

        for a in range(3):
            for b in range(3):
                dst[pl.ds((a * 3 + b) * C, C), :] = wacc[a * C:(a + 1) * C, b * C:(b + 1) * C].T

    def spread(src, buf, i):
        buf[me] = src[...]

        @pl.loop(1, ndev)
        def _(k):
            d = lax.rem(me + k, ndev)
            pltpu.make_async_remote_copy(src, buf.at[me], ss.at[i], sr.at[i], device_id=(d // nh, d % nh),
                                         device_id_type=MESH).start()

    def gather(buf, i):
        part = buf.at[pl.ds(0, ndev - 1)]
        pltpu.make_async_copy(part, part, sr.at[i]).wait()
        pltpu.make_async_copy(part, part, ss.at[i]).wait()
        s = buf[0]
        for k in range(1, ndev):
            s = s + buf[k]
        return s

    core, q_me = h % 2, h // 2
    half, piece = NT * C // 2, NT * C // SL

    def rcopy(src, dst, i, k, dev):
        return pltpu.make_async_remote_copy(src, dst, rs.at[i, k], rr.at[i, k], device_id=dev, device_id_type=MESH)

    outs = (dw1_ref, dw2_ref)

    def at(ref, start, n):
        return ref.at[pl.ds(pl.multiple_of(start, TB), n)]

    def ar_pair(i):
        other = 1 - core
        return rcopy(at(dwl.at[i], other * half, half), rd.at[i], i, 0, (w, h + 1 - 2 * core))

    def ar_xy(i):
        cps = []
        for k in range(1, 4):
            qo = q_me ^ k
            cps.append(rcopy(at(dwl.at[i], core * half + qo * piece, piece), rxy.at[i, k - 1], i, k, (w, qo * 2 + core)))
        return cps

    def ar_z(i):
        return [rcopy(zb.at[i, w], zb.at[i, w], i, 3 + k, (lax.rem(w + k, nw), h)) for k in range(1, nw)]

    def ar_z_in(i):
        return [rcopy(zb.at[i, w], zb.at[i, lax.rem(w + nw - k, nw)], i, 3 + k, (w, h)) for k in range(1, nw)]

    def ar_xy2(i):
        mine = at(outs[i], core * half + q_me * piece, piece)
        return [rcopy(mine, mine, i, 6 + k, (w, (q_me ^ k) * 2 + core)) for k in range(1, 4)]

    def ar_xy2_in(i):
        mine = at(outs[i], core * half + q_me * piece, piece)
        return [rcopy(mine, at(outs[i], core * half + (q_me ^ k) * piece, piece), i, 6 + k, (w, h)) for k in range(1, 4)]

    def ar_pair2(i):
        mine = at(outs[i], core * half, half)
        return rcopy(mine, mine, i, 10, (w, h + 1 - 2 * core))

    def ar_pair2_in(i):
        mine = at(outs[i], core * half, half)
        return rcopy(mine, at(outs[i], (1 - core) * half, half), i, 10, (w, h))

    def ar_step(i, n):
        if n == 0:
            ar_pair(i).start()
        elif n == 1:
            ar_pair(i).wait()
            for k in range(4):
                s = pl.ds(pl.multiple_of(core * half + k * piece, TB), piece)
                dwl[i, s, :] = dwl[i, s, :] + rd[i, pl.ds(k * piece, piece), :]
            for c in ar_xy(i):
                c.start()
        elif n == 2:
            for c in ar_xy(i):
                c.wait()
            s = pl.ds(pl.multiple_of(core * half + q_me * piece, TB), piece)
            zb[i, w] = dwl[i, s, :] + rxy[i, 0] + rxy[i, 1] + rxy[i, 2]
            for c in ar_z(i):
                c.start()
        elif n == 3:
            for c in ar_z(i):
                c.wait_send()
            for c in ar_z_in(i):
                c.wait_recv()
            s = zb[i, 0]
            for k in range(1, nw):
                s = s + zb[i, k]
            outs[i][pl.ds(pl.multiple_of(core * half + q_me * piece, TB), piece), :] = s
            for c in ar_xy2(i):
                c.start()
        elif n == 4:
            for c in ar_xy2(i):
                c.wait_send()
            for c in ar_xy2_in(i):
                c.wait_recv()
            ar_pair2(i).start()
        else:
            ar_pair2(i).wait_send()
            ar_pair2_in(i).wait_recv()

    okl = oks()
    loads[0].wait()
    build(xv, ucat, 0, None)
    weights(w1v, wc1, wt1)
    pl.semaphore_wait(barrier, ndev - 1)
    halo(0, xv, ec.at[0], hr.at[0], hc.at[0], hk.at[0], True)
    loads[1].wait()
    build(gv, gcat, 1, gt)
    halo(1, gv, ec.at[1], hr.at[1], hc.at[1], hk.at[1], True)
    weights(w2v, wc2, wt2)
    halo(0, xv, ec.at[0], hr.at[0], hc.at[0], hk.at[0], False)
    halo_rows(ucat, okl, lambda v: v[0], [hr.at[0]], [hc.at[0]], [hk.at[0]])

    def fin_a(q, o, carry):
        s1, s2 = carry
        for i, v in enumerate(rows_of(o)):
            vb = v.astype(BF)
            av[4 * q + i] = vb
            vf = vb.astype(F32)
            ec[2, 0, pl.ds(4 * q + i, 1), :] = vf[0:1, :]
            ec[2, 1, pl.ds(4 * q + i, 1), :] = vf[tw - 1:tw, :]
            s1 = s1 + _fold(vf)
            s2 = s2 + _fold(vf * vf)
        return s1, s2

    z8 = jnp.zeros((SL, C), F32)
    s1, s2 = conv(ucat, wc1, 0, th // 4, (z8, z8), fin_a)
    st[0:1, :] = s1.sum(0, keepdims=True)
    st[1:2, :] = s2.sum(0, keepdims=True)
    spread(st, sbuf, 0)
    halo(2, av, ec.at[2], hr.at[2], hc.at[2], hk.at[2], True)

    halo(1, gv, ec.at[1], hr.at[1], hc.at[1], hk.at[1], False)
    halo_rows(gcat, okl, lambda v: v[0], [hr.at[1]], [hc.at[1]], [hk.at[1]])

    def fin_dz(q, o, carry):
        for i, v in enumerate(rows_of(o)):
            dn[4 * q + i] = v
        return carry

    conv(gcat, wt2, 0, th // 4, 0, fin_dz)

    tot = _group_sum(gather(sbuf, 0)) / cnt
    mean = tot[0:1, :]
    rstd = lax.rsqrt(tot[1:2, :] - mean * mean + EPS)
    sh = -mean * rstd
    gam = gam_ref[...]
    bet = bet_ref[...]

    def act(a):
        xh = a * rstd + sh
        n = xh * gam + bet
        n2 = n * n
        p = 0.5 + 0.5 * jnp.tanh(n * (GC + GC2 * n2))
        return xh, n2, p, n * p

    def zrow(r, carry):
        t0, t1 = carry
        for j in range(0, tw, RB):
            s = pl.ds(j, RB)
            xh, n2, p, z = act(av[r, s, :].astype(F32))
            row[pl.ds(SL + j, RB), :] = z
            d = dn[r, s, :] * (p + z * (1.0 - p) * (2.0 * GC + 6.0 * GC2 * n2))
            dn[r, s, :] = d
            if j == 0:
                ec[3, 0, pl.ds(r, 1), :] = d[0:1, :]
            if j + RB == tw:
                ec[3, 1, pl.ds(r, 1), :] = d[63:RB, :]
            t0 = t0 + _fold(d * xh)
            t1 = t1 + _fold(d)
        cat_row(zcat, r + 1)
        return t0, t1

    t0, t1 = lax.fori_loop(0, th, zrow, (z8, z8))
    tt[0:1, :] = t0.sum(0, keepdims=True)
    tt[1:2, :] = t1.sum(0, keepdims=True)
    spread(tt, tbuf, 1)
    halo(3, dn, ec.at[3], hrd, hcd, hkd, True)

    halo(2, av, ec.at[2], hr.at[2], hc.at[2], hk.at[2], False)
    halo_rows(zcat, okl, lambda v: act(v[0])[3], [hr.at[2]], [hc.at[2]], [hk.at[2]])

    wgrad(gt, zcat, dwl.at[1])
    ar_step(1, 0)

    t = gather(tbuf, 1)
    dgam_ref[...] = t[0:1, :]
    dbet_ref[...] = t[1:2, :]
    u = _group_sum(t * gam) / cnt
    k1 = gam * rstd
    k2 = -rstd * rstd * u[0:1, :]
    k3 = -rstd * (u[1:2, :] + sh * u[0:1, :])

    @pl.loop(0, th)
    def _(r):
        for j in range(0, tw, RB):
            s = pl.ds(j, RB)
            v = dn[r, s, :] * k1 + av[r, s, :].astype(F32) * k2 + k3
            row[pl.ds(SL + j, RB), :] = v
        cat_row(gcat, r + 1)
        dat[r + 1] = gcat[r + 1, :, C:2 * C].T

    halo(3, dn, ec.at[3], hrd, hcd, hkd, False)
    halo_rows(gcat, okl, lambda v: v[0] * k1 + v[1] * k2 + k3, [hrd, hr.at[2]], [hcd, hc.at[2]], [hkd, hk.at[2]])
    ar_step(1, 1)

    wgrad(dat, ucat, dwl.at[0])
    ar_step(0, 0)
    ar_step(1, 2)

    def fin_dx(q, o, carry):
        for i, v in enumerate(rows_of(o)):
            dx_ref[4 * q + i] = (v + gv[4 * q + i].astype(F32)).astype(BF)
        return carry

    def fin_y(q, o, carry):
        for i, v in enumerate(rows_of(o)):
            y_ref[4 * q + i] = (v + xv[4 * q + i].astype(F32)).astype(BF)
        return carry

    n4 = th // 4
    conv(gcat, wt1, 0, n4 // 2, 0, fin_dx)
    ar_step(0, 1)
    ar_step(1, 3)
    conv(gcat, wt1, n4 // 2, n4, 0, fin_dx)
    ar_step(0, 2)
    ar_step(1, 4)
    conv(zcat, wc2, 0, n4, 0, fin_y)
    ar_step(0, 3)
    ar_step(1, 5)
    ar_step(0, 4)
    ar_step(0, 5)


def _flush(n, *refs):
    cps = [pltpu.make_async_copy(refs[i], refs[n + i], refs[-1].at[i]) for i in range(n)]
    for c in cps:
        c.start()
    for c in cps:
        c.wait()


def solution(mesh):
    nh, nw = mesh.shape['h'], mesh.shape['w']
    tile = P(None, 'h', 'w', None)

    def body(x, w1, gamma, beta, w2, g):
        _, th, tw, c = x.shape
        hbm = pl.BlockSpec(memory_space=pltpu.HBM)
        vm = pl.BlockSpec(memory_space=pltpu.VMEM)
        V = pltpu.VMEM
        D = pltpu.SemaphoreType.DMA
        img = jax.ShapeDtypeStruct((th, tw, c), BF)
        wsh = jax.ShapeDtypeStruct((NT * c, c), F32)
        vec = jax.ShapeDtypeStruct((1, c), F32)
        cat = V((th + 2, tw, 3 * c), BF)
        ndev = nh * nw
        scratch = dict(
            xv=V((th, tw, c), BF), gv=V((th, tw, c), BF),
            wc1=V((12 * c, 2 * c), BF), wt1=V((12 * c, 2 * c), BF), wc2=V((12 * c, 2 * c), BF), wt2=V((12 * c, 2 * c), BF),
            ucat=cat, gcat=cat, zcat=cat, gt=V((th + 2, c, tw), BF), dat=V((th + 2, c, tw), BF),
            av=V((th, tw, c), BF), dn=V((th, tw, c), F32), row=V((tw + TB, c), F32),
            hr=V((3, 2, tw, c), BF), hc=V((3, 2, th, c), F32), hk=V((3, 4, TB, c), BF),
            hrd=V((2, tw, c), F32), hcd=V((2, th, c), F32), hkd=V((4, TB, c), F32), ec=V((4, 2, th, c), F32),
            st=V((2, c), F32), sbuf=V((ndev, 2, c), F32), tt=V((2, c), F32), tbuf=V((ndev, 2, c), F32),
            wacc=V((3 * c, 3 * c), F32), dwl=V((2, NT * c, c), F32), rd=V((2, NT * c // 2, c), F32),
            rxy=V((2, 3, NT * c // SL, c), F32), zb=V((2, nw, NT * c // SL, c), F32),
            ld=D((2,)), hs=D((4, SL)), hv=D((4, SL)), ss=D((2,)), sr=D((2,)), rs=D((2, 11)), rr=D((2, 11)),
        )
        res = pl.pallas_call(
            functools.partial(_kernel, nh, nw, th, tw),
            out_shape=(img, img, wsh, wsh, vec, vec),
            in_specs=[hbm] * 2 + [vm] * 4,
            out_specs=(vm,) * 6,
            scratch_shapes=list(scratch.values()),
            compiler_params=pltpu.CompilerParams(collective_id=0, has_side_effects=True, vmem_limit_bytes=48 << 20),
        )(x.reshape(th, tw, c), g.reshape(th, tw, c), w1.reshape(NT, c, c), w2.reshape(NT, c, c),
          gamma.reshape(1, c), beta.reshape(1, c))
        y, dx, dw1, dw2, dg, db = pl.pallas_call(
            functools.partial(_flush, len(res)),
            out_shape=(img, img, wsh, wsh, vec, vec),
            in_specs=[vm] * len(res),
            out_specs=(hbm,) * len(res),
            scratch_shapes=[D((len(res),))],
            compiler_params=pltpu.CompilerParams(vmem_limit_bytes=1 << 20),
        )(*res)
        return (y.reshape(x.shape), dx.reshape(x.shape), dw1.reshape(3, 3, c, c), dw2.reshape(3, 3, c, c),
                dg.reshape(c), db.reshape(c))

    return jax.shard_map(body, mesh=mesh, in_specs=(tile, P(), P(), P(), P(), tile),
                         out_specs=(tile, tile, P(), P(), P(), P()), check_vma=False)
```

```python
import functools

import jax
import jax.numpy as jnp
from jax import lax
from jax.experimental import pallas as pl
from jax.experimental.pallas import tpu as pltpu
from jax.sharding import PartitionSpec as P

MESH = pl.DeviceIdType.MESH
GROUPS = 32
EPS = 1e-5
RB, TB, NT, SL = 64, 16, 9, 8
C = 128
C2, C3, ZERO = 2 * C, 3 * C, 0.0
BF = jnp.bfloat16
F32 = jnp.float32
GC = 0.7978845608028654
GC2 = GC * 0.044715
DIRS = ((-1, 0), (1, 0), (0, -1), (0, 1), (-1, -1), (-1, 1), (1, -1), (1, 1))
OPP = (1, 0, 3, 2, 7, 6, 5, 4)


def _group_sum(v):
    lane = lax.broadcasted_iota(jnp.int32, v.shape, 1)
    v = v + jnp.where(lane % 2 == 0, pltpu.roll(v, C - 1, 1), pltpu.roll(v, 1, 1))
    return v + jnp.where(lane % 4 < 2, pltpu.roll(v, C - 2, 1), pltpu.roll(v, 2, 1))


def _fold(v):
    return v.reshape(v.shape[0] // SL, SL, C).sum(0)


def _fold_inner(v):
    it = lax.broadcasted_iota(jnp.int32, (SL, C), 0)
    return _fold(v[SL:-SL]) + jnp.where(it == 0, ZERO, v[:SL]) + jnp.where(it == SL - 1, ZERO, v[-SL:])


def _kernel(nh, nw, th, tw, x_hbm, g_hbm, w1v, w2v, gam_ref, bet_ref,
            y_ref, dx_ref, dw1_ref, dw2_ref, dgam_ref, dbet_ref,
            xv, gv, wc1, wt1, wc2, wt2, ucat, gcat, zcat, gt, dat, av, dn, row,
            hr, hc, hk, hrd, hcd, hkd, ec,
            st, sbuf, tt, tbuf, dwl, rd, rxy, zb,
            ld, hs, hv, ss, sr, rs, rr):
    w = lax.axis_index('w')
    h = lax.axis_index('h')
    ndev = nh * nw
    me = w * nh + h
    cnt = float(th * nh * tw * nw * (C // GROUPS))

    barrier = pltpu.get_barrier_semaphore()

    def others():
        for dw in range(nw - 1, -1, -1):
            for dh in range(nh - 1, -1, -1):
                if dw or dh:
                    yield lax.rem(w + dw, nw), h ^ dh

    for dev in others():
        pl.semaphore_signal(barrier, inc=1, device_id=dev, device_id_type=MESH)

    loads = [pltpu.make_async_copy(s, d, ld.at[i]) for i, (s, d) in enumerate(
        ((x_hbm, xv), (g_hbm, gv)))]
    for c in loads:
        c.start()

    def neighbour(d):
        dy, dx = DIRS[d]
        hh, ww = h + dy, w + dx
        ok = (hh >= 0) & (hh < nh) & (ww >= 0) & (ww < nw)
        return ok, (ww, hh)

    def bufs(t):
        return (hr.at[t], hc.at[t], hk.at[t]) if t < 3 else (hrd, hcd, hkd)

    def halo(t, rows, start):
        cols = ec.at[t]
        hrow, hcol, hcor = bufs(t)
        for d, (dy, dx) in enumerate(DIRS):
            ok, dev = neighbour(d)
            o = OPP[d]
            r = 0 if dy < 0 else th - 1
            if dx == 0:
                src, dst = rows.at[r], hrow.at[o]
            elif dy == 0:
                src, dst = cols.at[d - 2], hcol.at[o - 2]
            else:
                src, dst = rows.at[r, pl.ds(0 if dx < 0 else tw - TB, TB)], hcor.at[o - 4]
            cp = pltpu.make_async_remote_copy(src, dst, hs.at[t, d], hv.at[t, o], device_id=dev, device_id_type=MESH)
            if start:
                pl.when(ok)(cp.start)
            else:
                back = pltpu.make_async_remote_copy(
                    src, (hrow.at[d] if dx == 0 else hcol.at[d - 2] if dy == 0 else hcor.at[d - 4]),
                    hs.at[t, d], hv.at[t, d], device_id=dev, device_id_type=MESH)

                @pl.when(ok)
                def _():
                    back.wait_send()
                    back.wait_recv()

    okl = [neighbour(d)[0] for d in range(SL)]

    def first(v):
        return v[0]

    def cat_row(cat, r, shifts=(0, 1, 2)):
        for j in range(0, tw, RB):
            for b in shifts:
                cat[r, pl.ds(j, RB), pl.ds(b * C, C)] = row[pl.ds(SL - 1 + b + j, RB), :].astype(BF)

    def shifted(cat):
        @pl.loop(1, th + 1)
        def _(r):
            for j in range(0, tw, RB):
                row[pl.ds(SL + j, RB), :] = cat[r, pl.ds(j, RB), C:C2].astype(F32)
            cat_row(cat, r, (0, 2))

    def set_ends(left, right):
        row[7:SL, :] = left
        row[tw + SL:tw + NT, :] = right

    def patch(cat, r, left, right):
        it = lax.broadcasted_iota(jnp.int32, (TB, C), 0)
        a = cat[r, 0:TB, 0:C].astype(F32)
        cat[r, 0:TB, 0:C] = jnp.where(it == 0, left, a).astype(BF)
        b = cat[r, tw - TB:tw, C2:C3].astype(F32)
        cat[r, tw - TB:tw, C2:C3] = jnp.where(it == 15, right, b).astype(BF)

    def halo_rows(cat, f, *ts):
        hrow, hcol, hcor = zip(*[bufs(t) for t in ts])
        for e, r in ((0, 0), (1, th + 1)):
            for j in range(0, tw, RB):
                row[pl.ds(SL + j, RB), :] = jnp.where(okl[e], f([b[e, pl.ds(j, RB), :].astype(F32) for b in hrow]), ZERO)
            kl, kr = 2 * e, 2 * e + 1
            cl = f([b[kl].astype(F32) for b in hcor])
            cr = f([b[kr].astype(F32) for b in hcor])
            set_ends(jnp.where(okl[4 + kl], cl[15:TB, :], ZERO), jnp.where(okl[4 + kr], cr[0:1, :], ZERO))
            cat_row(cat, r)

        @pl.loop(0, th // SL)
        def _(k):
            r8 = pl.multiple_of(k * SL, SL)
            lf = jnp.where(okl[2], f([b[0, pl.ds(r8, SL), :].astype(F32) for b in hcol]), ZERO)
            rg = jnp.where(okl[3], f([b[1, pl.ds(r8, SL), :].astype(F32) for b in hcol]), ZERO)
            for i in range(SL):
                patch(cat, r8 + i + 1, lf[i:i + 1, :], rg[i:i + 1, :])

    def build(src, cat, t, vt):
        @pl.loop(0, th)
        def _(r):
            for j in range(0, tw, RB):
                row[pl.ds(SL + j, RB), :] = src[r, pl.ds(j, RB), :].astype(F32)
            ec[t, 0, pl.ds(r, 1), :] = row[SL:NT, :]
            ec[t, 1, pl.ds(r, 1), :] = row[tw + 7:tw + SL, :]
            cat_row(cat, r + 1)
            if vt is not None:
                vt[r + 2] = src[r].T

    def weights(wv, wc, wt):
        for r in range(4):
            for b in range(3):
                for t in range(2):
                    a = r - t
                    sl = (pl.ds((r * 3 + b) * C, C), pl.ds(t * C, C))
                    if 0 <= a < 3:
                        wc[sl] = wv[a * 3 + b]
                        wt[sl] = wv[(2 - a) * 3 + 2 - b].T
                    else:
                        wc[sl] = jnp.zeros((C, C), BF)
                        wt[sl] = jnp.zeros((C, C), BF)

    def dot(blocks, wc):
        lhs = jnp.concatenate([jnp.concatenate(list(b), axis=1) for b in blocks], axis=0)
        return jnp.dot(lhs, wc[...], preferred_element_type=F32)

    def conv(cat, wc, lo, hi, carry, fn):
        for r0 in range(lo, hi, SL):
            n = min(SL, hi - r0)
            o = dot([[cat[r0 + p + r] for r in range(4)] for p in range(0, n, 2)], wc)
            carry = fn(range(r0, r0 + n), o, carry)
        return carry

    def rows_of(o):
        return [o[(i // 2) * tw:(i // 2 + 1) * tw, (i % 2) * C:(i % 2 + 1) * C] for i in range(2 * o.shape[0] // tw)]

    def wgrad_ab(vt, cat, dst):
        for k in (0, 1, th + 2, th + 3):
            vt[k] = jnp.zeros((C, tw), BF)
        lhs = jnp.concatenate([
            jnp.concatenate([vt[i + 2 - a] for a in range(3)], axis=0) for i in range(th + 2)], axis=1)
        rhs = cat[:, :, pl.ds(0, C2)].reshape((th + 2) * tw, C2)
        o = jnp.dot(lhs, rhs, preferred_element_type=F32)
        for b in range(2):
            for a in range(3):
                dst[pl.ds((b * 3 + a) * C, C), :] = o[a * C:(a + 1) * C, b * C:(b + 1) * C].T

    def wgrad_c(vt, cat, dst):
        n = pl.ds(C2, C)
        rows = range(0, th + 2, 2)
        lhs = jnp.concatenate([jnp.concatenate([vt[i + r] for r in range(4)], axis=0) for i in rows], axis=1)
        rhs = jnp.concatenate([jnp.concatenate([cat[i, :, n], cat[i + 1, :, n]], axis=1) for i in rows], axis=0)
        o = jnp.dot(lhs, rhs, preferred_element_type=F32)
        for a in range(3):
            v = [o[(t + 2 - a) * C:(t + 3 - a) * C, t * C:(t + 1) * C] for t in range(2)]
            dst[pl.ds((6 + a) * C, C), :] = (v[0] + v[1]).T

    def spread(src, buf, i):
        buf[me] = src[...]
        for dev in others():
            pltpu.make_async_remote_copy(src, buf.at[me], ss.at[i], sr.at[i], device_id=dev, device_id_type=MESH).start()

    def gather(buf, i):
        part = buf.at[pl.ds(0, ndev - 1)]
        pltpu.make_async_copy(part, part, sr.at[i]).wait()
        pltpu.make_async_copy(part, part, ss.at[i]).wait()
        s = buf[0]
        for k in range(1, ndev):
            s = s + buf[k]
        return s

    core, q_me = h % 2, h // 2
    jobs = ((0, 0, 6 * C), (0, 6 * C, C3), (1, 0, NT * C))
    outs = (dw1_ref, dw2_ref)

    def ar_step(i, n):
        k_arr, base, rows = jobs[i]
        src, out = dwl.at[k_arr], outs[k_arr]
        half, piece = rows // 2, rows // 8
        buf = pl.ds(0, piece)

        def sl(c, q=0, n=piece):
            return pl.ds(pl.multiple_of(base + c * half + q * piece, SL), n)

        def cp(a, b, k, dev):
            return pltpu.make_async_remote_copy(a, b, rs.at[i, k], rr.at[i, k], device_id=dev, device_id_type=MESH)

        peer = (w, h ^ 1)
        xy = [(k, (w, h ^ (2 * k))) for k in range(1, 4)]
        zs = [(k, lax.rem(w + k, nw), lax.rem(w + nw - k, nw)) for k in range(1, nw)]
        mine = sl(core, q_me)
        pair_rs = cp(src.at[sl(1 - core, 0, half)], rd.at[i, pl.ds(0, half)], 0, peer)
        xy_rs = [cp(src.at[sl(core, q_me ^ k)], rxy.at[i, k - 1, buf], k, dev) for k, dev in xy]
        zslot = zb.at[i, w, buf]
        z_out = [cp(zslot, zslot, 3 + k, (to, h)) for k, to, _ in zs]
        z_in = [cp(zslot, zb.at[i, fr, buf], 3 + k, peer) for k, _, fr in zs]
        xy_out = [cp(out.at[mine], out.at[mine], 6 + k, dev) for k, dev in xy]
        xy_in = [cp(out.at[mine], out.at[sl(core, q_me ^ k)], 6 + k, peer) for k, _ in xy]
        own = out.at[sl(core, 0, half)]
        pair_out = cp(own, own, 10, peer)
        pair_in = cp(own, out.at[sl(1 - core, 0, half)], 10, peer)

        def begin(cps):
            for c in cps:
                c.start()

        def end(sent, got):
            for c in sent:
                c.wait_send()
            for c in got:
                c.wait_recv()

        if n == 0:
            begin([pair_rs])
        elif n == 1:
            end([pair_rs], [pair_rs])
            for k in range(4):
                src[sl(core, k), :] = src[sl(core, k), :] + rd[i, pl.ds(k * piece, piece), :]
            begin(xy_rs)
        elif n == 2:
            end(xy_rs, xy_rs)
            zb[i, w, buf] = src[mine, :] + rxy[i, 0, buf] + rxy[i, 1, buf] + rxy[i, 2, buf]
            begin(z_out)
        elif n == 3:
            end(z_out, z_in)
            v = zb[i, 0, buf]
            for k in range(1, nw):
                v = v + zb[i, k, buf]
            out[mine, :] = v
            begin(xy_out)
        elif n == 4:
            end(xy_out, xy_in)
            begin([pair_out])
        else:
            end([pair_out], [pair_in])

    z8 = jnp.zeros((SL, C), F32)
    set_ends(z8[0:1], z8[0:1])
    weights(w1v, wc1, wt1)
    loads[0].wait()
    build(xv, ucat, 0, None)

    def fin_a(rows, o, carry):
        s1, s2 = carry
        for r, v in zip(rows, rows_of(o)):
            vb = v.astype(BF)
            av[r] = vb
            vf = vb.astype(F32)
            s1 = s1 + _fold_inner(vf)
            s2 = s2 + _fold_inner(vf * vf)
        return s1, s2

    sums = conv(ucat, wc1, 2, th // 2 + 2, (z8, z8), fin_a)
    pl.semaphore_wait(barrier, ndev - 1)
    halo(0, xv, True)
    sums = conv(ucat, wc1, th // 2 + 2, th - 2, sums, fin_a)

    weights(w2v, wc2, wt2)
    loads[1].wait()
    build(gv, gcat, 1, gt)
    halo(1, gv, True)

    halo(0, xv, False)
    halo_rows(ucat, first, 0)
    o = dot([[ucat[p + r] for r in range(4)] for p in (0, th - 2)], wc1)
    s1, s2 = fin_a((0, 1, th - 2, th - 1), o, sums)
    it = lax.broadcasted_iota(jnp.int32, (TB, C), 0)
    sides = (pl.ds(0, TB), pl.ds(tw - TB, TB))
    o = dot([[ucat[p + r, s] for r in range(4)] for p in range(0, th, 2) for s in sides], wc1)
    for p in range(th):
        for e, s in enumerate(sides):
            k = (p // 2) * 2 + e
            vb = o[k * TB:(k + 1) * TB, (p % 2) * C:(p % 2 + 1) * C].astype(BF)
            av[p, s] = vb
            vf = jnp.where(it == e * (TB - 1), vb.astype(F32), ZERO)
            ec[2, e, p:p + 1, :] = vf[e * (TB - 1):e * (TB - 1) + 1, :]
            s1 = s1 + _fold(vf)
            s2 = s2 + _fold(vf * vf)
    st[0:1, :] = s1.sum(0, keepdims=True)
    st[1:2, :] = s2.sum(0, keepdims=True)
    spread(st, sbuf, 0)
    halo(2, av, True)

    halo(1, gv, False)
    halo_rows(gcat, first, 1)

    def fin_dz(rows, o, carry):
        for r, v in zip(rows, rows_of(o)):
            dn[r] = v
        return carry

    conv(gcat, wt2, 0, th, 0, fin_dz)

    tot = _group_sum(gather(sbuf, 0)) / cnt
    mean = tot[0:1, :]
    rstd = lax.rsqrt(tot[1:2, :] - mean * mean + EPS)
    sh = -mean * rstd
    gam = gam_ref[...]
    bet = bet_ref[...]

    def act(a):
        xh = a * rstd + sh
        n = xh * gam + bet
        n2 = n * n
        p = 0.5 + 0.5 * jnp.tanh(n * (GC + GC2 * n2))
        return xh, n2, p, n * p

    def zrow(r, carry):
        t0, t1 = carry
        for j in range(0, tw, RB):
            s = pl.ds(j, RB)
            xh, n2, p, z = act(av[r, s, :].astype(F32))
            zcat[r + 1, s, C:C2] = z.astype(BF)
            d = dn[r, s, :] * (p + z * (1.0 - p) * (2.0 * GC + 6.0 * GC2 * n2))
            dn[r, s, :] = d
            if j == 0:
                ec[3, 0, pl.ds(r, 1), :] = d[0:1, :]
            if j + RB == tw:
                ec[3, 1, pl.ds(r, 1), :] = d[RB - 1:RB, :]
            t0 = t0 + _fold(d * xh)
            t1 = t1 + _fold(d)
        return t0, t1

    t0, t1 = lax.fori_loop(0, th, zrow, (z8, z8))
    tt[0:1, :] = t0.sum(0, keepdims=True)
    tt[1:2, :] = t1.sum(0, keepdims=True)
    spread(tt, tbuf, 1)
    halo(3, dn, True)

    shifted(zcat)
    halo(2, av, False)
    halo_rows(zcat, lambda v: act(v[0])[3], 2)
    wgrad_ab(gt, zcat, dwl.at[1])
    wgrad_c(gt, zcat, dwl.at[1])
    ar_step(2, 0)

    t = gather(tbuf, 1)
    dgam_ref[...] = t[0:1, :]
    dbet_ref[...] = t[1:2, :]
    u = _group_sum(t * gam) / cnt
    k1 = gam * rstd
    k2 = -rstd * rstd * u[0:1, :]
    k3 = -rstd * (u[1:2, :] + sh * u[0:1, :])

    @pl.loop(0, th)
    def _(r):
        for j in range(0, tw, RB):
            s = pl.ds(j, RB)
            v = (dn[r, s, :] * k1 + av[r, s, :].astype(F32) * k2 + k3).astype(BF)
            gcat[r + 1, s, C:C2] = v
        dat[r + 2] = gcat[r + 1, :, C:C2].T

    ar_step(2, 1)

    wgrad_ab(dat, ucat, dwl.at[0])
    ar_step(0, 0)
    wgrad_c(dat, ucat, dwl.at[0])
    ar_step(0, 1)
    ar_step(1, 0)
    ar_step(2, 2)

    shifted(gcat)
    halo(3, dn, False)
    halo_rows(gcat, lambda v: v[0] * k1 + v[1] * k2 + k3, 3, 2)
    ar_step(1, 1)

    def fin_dx(rows, o, carry):
        for r, v in zip(rows, rows_of(o)):
            dx_ref[r] = (v + gv[r].astype(F32)).astype(BF)
        return carry

    def fin_y(rows, o, carry):
        for r, v in zip(rows, rows_of(o)):
            y_ref[r] = (v + xv[r].astype(F32)).astype(BF)
        return carry

    conv(gcat, wt1, 0, th, 0, fin_dx)
    ar_step(2, 3)
    ar_step(0, 2)
    conv(zcat, wc2, 0, th // 4, 0, fin_y)
    ar_step(1, 2)
    conv(zcat, wc2, th // 4, th, 0, fin_y)
    ar_step(2, 4)
    for n in range(3, 6):
        ar_step(0, n)
        ar_step(1, n)
        if n == 3:
            ar_step(2, 5)


def _flush(n, *refs):
    ins, res, sem = refs[:n], refs[n:2 * n], refs[-1]
    cps = []
    for i in range(n):
        if res[i].shape == ins[i].shape:
            cps.append((ins[i], res[i]))
        else:
            cps += [(ins[i].at[pl.ds((k % 3 * 3 + k // 3) * C, C)], res[i].at[k]) for k in range(NT)]
    cps = [pltpu.make_async_copy(a, b, sem.at[k]) for k, (a, b) in enumerate(cps)]
    for c in cps:
        c.start()
    for c in cps:
        c.wait()


def solution(mesh):
    nh, nw = mesh.shape['h'], mesh.shape['w']
    tile = P(None, 'h', 'w', None)

    def body(x, w1, gamma, beta, w2, g):
        _, th, tw, c = x.shape
        hbm = pl.BlockSpec(memory_space=pltpu.HBM)
        vm = pl.BlockSpec(memory_space=pltpu.VMEM)
        V = pltpu.VMEM
        D = pltpu.SemaphoreType.DMA
        img = jax.ShapeDtypeStruct((th, tw, c), BF)
        wsh = jax.ShapeDtypeStruct((NT * c, c), F32)
        wsp = jax.ShapeDtypeStruct((NT, c, c), F32)
        vec = jax.ShapeDtypeStruct((1, c), F32)
        cat = V((th + 2, tw, 3 * c), BF)
        ndev = nh * nw
        scratch = dict(
            xv=V((th, tw, c), BF), gv=V((th, tw, c), BF),
            wc1=V((12 * c, 2 * c), BF), wt1=V((12 * c, 2 * c), BF), wc2=V((12 * c, 2 * c), BF), wt2=V((12 * c, 2 * c), BF),
            ucat=cat, gcat=cat, zcat=cat, gt=V((th + 4, c, tw), BF), dat=V((th + 4, c, tw), BF),
            av=V((th, tw, c), BF), dn=V((th, tw, c), F32), row=V((tw + TB, c), F32),
            hr=V((3, 2, tw, c), BF), hc=V((3, 2, th, c), F32), hk=V((3, 4, TB, c), BF),
            hrd=V((2, tw, c), F32), hcd=V((2, th, c), F32), hkd=V((4, TB, c), F32), ec=V((4, 2, th, c), F32),
            st=V((2, c), F32), sbuf=V((ndev, 2, c), F32), tt=V((2, c), F32), tbuf=V((ndev, 2, c), F32),
            dwl=V((2, NT * c, c), F32),
            rd=V((3, NT * c // 2, c), F32), rxy=V((3, 3, NT * c // SL, c), F32), zb=V((3, nw, NT * c // SL, c), F32),
            ld=D((2,)), hs=D((4, SL)), hv=D((4, SL)), ss=D((2,)), sr=D((2,)), rs=D((3, 11)), rr=D((3, 11)),
        )
        res = pl.pallas_call(
            functools.partial(_kernel, nh, nw, th, tw),
            out_shape=(img, img, wsh, wsh, vec, vec),
            in_specs=[hbm] * 2 + [vm] * 4,
            out_specs=(vm,) * 6,
            scratch_shapes=list(scratch.values()),
            compiler_params=pltpu.CompilerParams(collective_id=0, has_side_effects=True, vmem_limit_bytes=48 << 20),
        )(x.reshape(th, tw, c), g.reshape(th, tw, c), w1.reshape(NT, c, c), w2.reshape(NT, c, c),
          gamma.reshape(1, c), beta.reshape(1, c))
        y, dx, dw1, dw2, dg, db = pl.pallas_call(
            functools.partial(_flush, len(res)),
            out_shape=(img, img, wsp, wsp, vec, vec),
            in_specs=[vm] * len(res),
            out_specs=(hbm,) * len(res),
            scratch_shapes=[D((4 + 2 * NT,))],
            compiler_params=pltpu.CompilerParams(vmem_limit_bytes=1 << 20),
        )(*res)
        return (y.reshape(x.shape), dx.reshape(x.shape), dw1.reshape(3, 3, c, c), dw2.reshape(3, 3, c, c),
                dg.reshape(c), db.reshape(c))

    return jax.shard_map(body, mesh=mesh, in_specs=(tile, P(), P(), P(), P(), tile),
                         out_specs=(tile, tile, P(), P(), P(), P()), check_vma=False)
```

```python
import functools

import jax
import jax.numpy as jnp
from jax import lax
from jax.experimental import pallas as pl
from jax.experimental.pallas import tpu as pltpu
from jax.sharding import PartitionSpec as P

MESH = pl.DeviceIdType.MESH
GROUPS = 32
EPS = 1e-5
RB, TB, NT, SL = 64, 16, 9, 8
C = 128
C2, C3, ZERO = 2 * C, 3 * C, 0.0
BF = jnp.bfloat16
F32 = jnp.float32
GC = 0.7978845608028654
GC2 = GC * 0.044715
DIRS = ((-1, 0), (1, 0), (0, -1), (0, 1), (-1, -1), (-1, 1), (1, -1), (1, 1))
OPP = (1, 0, 3, 2, 7, 6, 5, 4)


def _group_sum(v):
    lane = lax.broadcasted_iota(jnp.int32, v.shape, 1)
    v = v + jnp.where(lane % 2 == 0, pltpu.roll(v, C - 1, 1), pltpu.roll(v, 1, 1))
    return v + jnp.where(lane % 4 < 2, pltpu.roll(v, C - 2, 1), pltpu.roll(v, 2, 1))


def _fold(v):
    return v.reshape(v.shape[0] // SL, SL, C).sum(0)


def _fold_inner(v):
    it = lax.broadcasted_iota(jnp.int32, (SL, C), 0)
    return _fold(v[SL:-SL]) + jnp.where(it == 0, ZERO, v[:SL]) + jnp.where(it == SL - 1, ZERO, v[-SL:])


def _kernel(nh, nw, th, tw, x_hbm, g_hbm, w1v, w2v, gam_ref, bet_ref,
            y_ref, dx_ref, dw1_ref, dw2_ref, dgam_ref, dbet_ref,
            xv, gv, wc1, wt1, wc2, wt2, ucat, gcat, zcat, gt, dat, av, dn, row,
            hr, hc, hk, hrd, hcd, hkd, ec,
            st, sbuf, tt, tbuf, dwl, rd, rxy, zx_buf,
            ld, hs, hv, ss, sr, rs, rr):
    w = lax.axis_index('w')
    h = lax.axis_index('h')
    ndev = nh * nw
    me = w * nh + h
    cnt = float(th * nh * tw * nw * (C // GROUPS))

    barrier = pltpu.get_barrier_semaphore()

    def others():
        for dw in range(nw - 1, -1, -1):
            for dh in range(nh - 1, -1, -1):
                if dw or dh:
                    yield lax.rem(w + dw, nw), h ^ dh

    for dev in others():
        pl.semaphore_signal(barrier, inc=1, device_id=dev, device_id_type=MESH)

    loads = [pltpu.make_async_copy(s, d, ld.at[i]) for i, (s, d) in enumerate(
        ((x_hbm, xv), (g_hbm, gv)))]
    for c in loads:
        c.start()

    def neighbour(d):
        dy, dx = DIRS[d]
        hh, ww = h + dy, w + dx
        ok = (hh >= 0) & (hh < nh) & (ww >= 0) & (ww < nw)
        return ok, (ww, hh)

    def bufs(t):
        return (hr.at[t], hc.at[t], hk.at[t]) if t < 3 else (hrd, hcd, hkd)

    def halo(t, rows, start):
        cols = ec.at[t]
        hrow, hcol, hcor = bufs(t)
        for d, (dy, dx) in enumerate(DIRS):
            ok, dev = neighbour(d)
            o = OPP[d]
            r = 0 if dy < 0 else rows.shape[0] - 1
            if dx == 0:
                src, dst = rows.at[r], hrow.at[o]
            elif dy == 0:
                src, dst = cols.at[d - 2], hcol.at[o - 2]
            else:
                src, dst = rows.at[r, pl.ds(0 if dx < 0 else tw - TB, TB)], hcor.at[o - 4]
            cp = pltpu.make_async_remote_copy(src, dst, hs.at[t, d], hv.at[t, o], device_id=dev, device_id_type=MESH)
            if start:
                pl.when(ok)(cp.start)
            else:
                back = pltpu.make_async_remote_copy(
                    src, (hrow.at[d] if dx == 0 else hcol.at[d - 2] if dy == 0 else hcor.at[d - 4]),
                    hs.at[t, d], hv.at[t, d], device_id=dev, device_id_type=MESH)

                @pl.when(ok)
                def _():
                    back.wait_send()
                    back.wait_recv()

    okl = [neighbour(d)[0] for d in range(SL)]

    def first(v):
        return v[0]

    def cat_row(cat, r, shifts=(0, 1, 2)):
        for j in range(0, tw, RB):
            for b in shifts:
                cat[r, pl.ds(j, RB), pl.ds(b * C, C)] = row[pl.ds(SL - 1 + b + j, RB), :].astype(BF)

    def shifted(cat):
        @pl.loop(1, th + 1)
        def _(r):
            for j in range(0, tw, RB):
                row[pl.ds(SL + j, RB), :] = cat[r, pl.ds(j, RB), C:C2].astype(F32)
            cat_row(cat, r, (0, 2))

    def set_ends(left, right):
        row[7:SL, :] = left
        row[tw + SL:tw + NT, :] = right

    def patch(cat, r, left, right):
        it = lax.broadcasted_iota(jnp.int32, (TB, C), 0)
        a = cat[r, 0:TB, 0:C].astype(F32)
        cat[r, 0:TB, 0:C] = jnp.where(it == 0, left, a).astype(BF)
        b = cat[r, tw - TB:tw, C2:C3].astype(F32)
        cat[r, tw - TB:tw, C2:C3] = jnp.where(it == 15, right, b).astype(BF)

    def halo_rows(cat, f, *ts):
        hrow, hcol, hcor = zip(*[bufs(t) for t in ts])
        for e, r in ((0, 0), (1, th + 1)):
            for j in range(0, tw, RB):
                row[pl.ds(SL + j, RB), :] = jnp.where(okl[e], f([b[e, pl.ds(j, RB), :].astype(F32) for b in hrow]), ZERO)
            kl, kr = 2 * e, 2 * e + 1
            cl = f([b[kl].astype(F32) for b in hcor])
            cr = f([b[kr].astype(F32) for b in hcor])
            set_ends(jnp.where(okl[4 + kl], cl[15:TB, :], ZERO), jnp.where(okl[4 + kr], cr[0:1, :], ZERO))
            cat_row(cat, r)

        @pl.loop(0, th // SL)
        def _(k):
            r8 = pl.multiple_of(k * SL, SL)
            lf = jnp.where(okl[2], f([b[0, pl.ds(r8, SL), :].astype(F32) for b in hcol]), ZERO)
            rg = jnp.where(okl[3], f([b[1, pl.ds(r8, SL), :].astype(F32) for b in hcol]), ZERO)
            for i in range(SL):
                patch(cat, r8 + i + 1, lf[i:i + 1, :], rg[i:i + 1, :])

    def build(src, cat, t):
        @pl.loop(0, th)
        def _(r):
            for j in range(0, tw, RB):
                row[pl.ds(SL + j, RB), :] = src[r, pl.ds(j, RB), :].astype(F32)
            ec[t, 0, pl.ds(r, 1), :] = row[SL:NT, :]
            ec[t, 1, pl.ds(r, 1), :] = row[tw + SL - 1:tw + SL, :]
            cat_row(cat, r + 1)

    def weights(wv, wc, flip):
        for r in range(4):
            for b in range(3):
                for t in range(2):
                    k = (r - t) * 3 + b
                    ok = t <= r < t + 3
                    v = jnp.zeros((C, C), BF) if not ok else wv[NT - 1 - k].T if flip else wv[k]
                    wc[pl.ds((r * 3 + b) * C, C), pl.ds(t * C, C)] = v

    def dot(blocks, wc):
        lhs = jnp.concatenate([jnp.concatenate(list(b), axis=1) for b in blocks], axis=0)
        return jnp.dot(lhs, wc[...], preferred_element_type=F32)

    def conv(cat, wc, lo, hi, carry, fn):
        for r0 in range(lo, hi, SL):
            n = min(SL, hi - r0)
            o = dot([[cat[r0 + p + r] for r in range(4)] for p in range(0, n, 2)], wc)
            carry = fn(range(r0, r0 + n), o, carry)
        return carry

    def rows_of(o):
        return [o[(i // 2) * tw:(i // 2 + 1) * tw, (i % 2) * C:(i % 2 + 1) * C] for i in range(2 * o.shape[0] // tw)]

    def wgrad_ab(vt, cat, dst):
        for k in (0, 1, th + 2, th + 3):
            vt[k] = jnp.zeros((C, tw), BF)
        lhs = jnp.concatenate([
            jnp.concatenate([vt[i + 2 - a] for a in range(3)], axis=0) for i in range(th + 2)], axis=1)
        rhs = cat[:, :, pl.ds(0, C2)].reshape((th + 2) * tw, C2)
        o = jnp.dot(lhs, rhs, preferred_element_type=F32)
        for b in range(2):
            for a in range(3):
                dst[pl.ds((b * 3 + a) * C, C), :] = o[a * C:(a + 1) * C, b * C:(b + 1) * C].T

    def wgrad_c(vt, cat, dst):
        n = pl.ds(C2, C)
        rows = range(0, th + 2, 2)
        lhs = jnp.concatenate([jnp.concatenate([vt[i + r] for r in range(4)], axis=0) for i in rows], axis=1)
        rhs = jnp.concatenate([jnp.concatenate([cat[i, :, n], cat[i + 1, :, n]], axis=1) for i in rows], axis=0)
        o = jnp.dot(lhs, rhs, preferred_element_type=F32)
        for a in range(3):
            v = [o[(t + 2 - a) * C:(t + 3 - a) * C, t * C:(t + 1) * C] for t in range(2)]
            dst[pl.ds((6 + a) * C, C), :] = (v[0] + v[1]).T

    def spread(src, buf, i):
        buf[me] = src[...]
        for dev in others():
            pltpu.make_async_remote_copy(src, buf.at[me], ss.at[i], sr.at[i], device_id=dev, device_id_type=MESH).start()

    def gather(buf, i):
        part = buf.at[pl.ds(0, ndev - 1)]
        pltpu.make_async_copy(part, part, sr.at[i]).wait()
        pltpu.make_async_copy(part, part, ss.at[i]).wait()
        s = buf[0]
        for k in range(1, ndev):
            s = s + buf[k]
        return s

    core, q_me = h % 2, h // 2
    jobs = ((0, 0, 6 * C), (0, 6 * C, C3), (1, 0, NT * C))
    outs = (dw1_ref, dw2_ref)

    def ar_step(i, n):
        k_arr, base, rows = jobs[i]
        src, out = dwl.at[k_arr], outs[k_arr]
        half, piece = rows // 2, rows // 8
        buf = pl.ds(0, piece)

        def sl(c, q=0, n=piece):
            return pl.ds(pl.multiple_of(base + c * half + q * piece, SL), n)

        def cp(a, b, k, dev):
            return pltpu.make_async_remote_copy(a, b, rs.at[i, k], rr.at[i, k], device_id=dev, device_id_type=MESH)

        peer = (w, h ^ 1)
        xy = [(k, (w, h ^ (2 * k))) for k in range(1, 4)]
        zp = [(k, lax.rem(w + k, nw), lax.rem(w + nw - k, nw)) for k in range(1, nw)]
        mine = sl(core, q_me)
        pair_rs = cp(src.at[sl(1 - core, 0, half)], rd.at[i, pl.ds(0, half)], 0, peer)
        xy_rs = [cp(src.at[sl(core, q_me ^ k)], rxy.at[i, k - 1, buf], k, dev) for k, dev in xy]
        zx = zx_buf.at[i]
        zx_out = [cp(zx.at[w, buf], zx.at[w, buf], 3 + k, (to, h)) for k, to, _ in zp]
        zx_in = [cp(zx.at[w, buf], zx.at[fr, buf], 3 + k, peer) for k, _, fr in zp]
        xy_out = [cp(out.at[mine], out.at[mine], 6 + k, dev) for k, dev in xy]
        xy_in = [cp(out.at[mine], out.at[sl(core, q_me ^ k)], 6 + k, peer) for k, _ in xy]
        own = out.at[sl(core, 0, half)]
        pair_out = cp(own, own, 10, peer)
        pair_in = cp(own, out.at[sl(1 - core, 0, half)], 10, peer)

        def begin(cps):
            for c in cps:
                c.start()

        def end(sent, got):
            for c in sent:
                c.wait_send()
            for c in got:
                c.wait_recv()

        if n == 0:
            begin([pair_rs])
        elif n == 1:
            end([pair_rs], [pair_rs])
            for k in range(4):
                src[sl(core, k), :] = src[sl(core, k), :] + rd[i, pl.ds(k * piece, piece), :]
            begin(xy_rs)
        elif n == 2:
            end(xy_rs, xy_rs)
            zx[w, buf] = src[mine, :] + rxy[i, 0, buf] + rxy[i, 1, buf] + rxy[i, 2, buf]
            begin(zx_out)
        elif n == 3:
            end(zx_out, zx_in)
            v = zx[0, buf]
            for k in range(1, nw):
                v = v + zx[k, buf]
            out[mine, :] = v
            begin(xy_out)
        elif n == 4:
            end(xy_out, xy_in)
            begin([pair_out])
        else:
            end([pair_out], [pair_in])

    z8 = jnp.zeros((SL, C), F32)
    set_ends(z8[0:1], z8[0:1])
    weights(w1v, wc1, False)
    loads[0].wait()
    build(xv, ucat, 0)

    def fin_a(rows, o, carry):
        s1, s2 = carry
        for r, v in zip(rows, rows_of(o)):
            vb = v.astype(BF)
            av[r] = vb
            vf = vb.astype(F32)
            s1 = s1 + _fold_inner(vf)
            s2 = s2 + _fold_inner(vf * vf)
        return s1, s2

    sums = conv(ucat, wc1, 2, th // 2 + 2, (z8, z8), fin_a)
    pl.semaphore_wait(barrier, ndev - 1)
    halo(0, xv, True)
    sums = conv(ucat, wc1, th // 2 + 2, th - 2, sums, fin_a)

    weights(w2v, wt2, True)
    loads[1].wait()
    build(gv, gcat, 1)
    halo(1, gv, True)

    halo(0, xv, False)
    halo_rows(ucat, first, 0)
    o = dot([[ucat[p + r] for r in range(4)] for p in (0, th - 2)], wc1)
    s1, s2 = fin_a((0, 1, th - 2, th - 1), o, sums)
    it = lax.broadcasted_iota(jnp.int32, (TB, C), 0)
    sides = (pl.ds(0, TB), pl.ds(tw - TB, TB))
    o = dot([[ucat[p + r, s] for r in range(4)] for p in range(0, th, 2) for s in sides], wc1)
    for p in range(th):
        for e, s in enumerate(sides):
            k = (p // 2) * 2 + e
            vb = o[k * TB:(k + 1) * TB, (p % 2) * C:(p % 2 + 1) * C].astype(BF)
            av[p, s] = vb
            vf = jnp.where(it == e * (TB - 1), vb.astype(F32), ZERO)
            ec[2, e, p:p + 1, :] = vf[e * (TB - 1):e * (TB - 1) + 1, :]
            s1 = s1 + _fold(vf)
            s2 = s2 + _fold(vf * vf)
    st[0:1, :] = s1.sum(0, keepdims=True)
    st[1:2, :] = s2.sum(0, keepdims=True)
    spread(st, sbuf, 0)
    halo(2, av, True)

    @pl.loop(0, th)
    def _(r):
        gt[r + 2] = gv[r].T

    halo(1, gv, False)
    halo_rows(gcat, first, 1)

    def fin_dz(rows, o, carry):
        for r, v in zip(rows, rows_of(o)):
            dn[r] = v
        return carry

    conv(gcat, wt2, 0, th, 0, fin_dz)

    tot = _group_sum(gather(sbuf, 0)) / cnt
    mean = tot[0:1, :]
    rstd = lax.rsqrt(tot[1:2, :] - mean * mean + EPS)
    sh = -mean * rstd
    gam = gam_ref[...]
    bet = bet_ref[...]

    def act(a):
        xh = a * rstd + sh
        n = xh * gam + bet
        n2 = n * n
        p = 0.5 + 0.5 * jnp.tanh(n * (GC + GC2 * n2))
        return xh, n2, p, n * p

    def zrow(r, carry):
        t0, t1 = carry
        for j in range(0, tw, RB):
            s = pl.ds(j, RB)
            xh, n2, p, z = act(av[r, s, :].astype(F32))
            zcat[r + 1, s, C:C2] = z.astype(BF)
            d = dn[r, s, :] * (p + z * (1.0 - p) * (2.0 * GC + 6.0 * GC2 * n2))
            dn[r, s, :] = d
            if j == 0:
                ec[3, 0, pl.ds(r, 1), :] = d[0:1, :]
            if j + RB == tw:
                ec[3, 1, pl.ds(r, 1), :] = d[RB - 1:RB, :]
            t0 = t0 + _fold(d * xh)
            t1 = t1 + _fold(d)
        return t0, t1

    t0, t1 = lax.fori_loop(0, th, zrow, (z8, z8))
    tt[0:1, :] = t0.sum(0, keepdims=True)
    tt[1:2, :] = t1.sum(0, keepdims=True)
    spread(tt, tbuf, 1)
    halo(3, dn, True)

    shifted(zcat)
    halo(2, av, False)
    halo_rows(zcat, lambda v: act(v[0])[3], 2)
    wgrad_ab(gt, zcat, dwl.at[1])
    wgrad_c(gt, zcat, dwl.at[1])
    ar_step(2, 0)

    t = gather(tbuf, 1)
    dgam_ref[...] = t[0:1, :]
    dbet_ref[...] = t[1:2, :]
    u = _group_sum(t * gam) / cnt
    k1 = gam * rstd
    k2 = -rstd * rstd * u[0:1, :]
    k3 = -rstd * (u[1:2, :] + sh * u[0:1, :])

    def da_rows(lo, hi):
        @pl.loop(lo, hi)
        def _(r):
            for j in range(0, tw, RB):
                s = pl.ds(j, RB)
                v = (dn[r, s, :] * k1 + av[r, s, :].astype(F32) * k2 + k3).astype(BF)
                gcat[r + 1, s, C:C2] = v
            dat[r + 2] = gcat[r + 1, :, C:C2].T

    da_rows(0, 3 * th // 4)
    ar_step(2, 1)
    da_rows(3 * th // 4, th)

    wgrad_ab(dat, ucat, dwl.at[0])
    ar_step(0, 0)
    wgrad_c(dat, ucat, dwl.at[0])
    ar_step(0, 1)
    ar_step(1, 0)
    weights(w1v, wt1, True)
    ar_step(2, 2)

    shifted(gcat)
    halo(3, dn, False)
    halo_rows(gcat, lambda v: v[0] * k1 + v[1] * k2 + k3, 3, 2)
    ar_step(1, 1)

    def fin_dx(rows, o, carry):
        for r, v in zip(rows, rows_of(o)):
            dx_ref[r] = (v + gv[r].astype(F32)).astype(BF)
        return carry

    def fin_y(rows, o, carry):
        for r, v in zip(rows, rows_of(o)):
            y_ref[r] = (v + xv[r].astype(F32)).astype(BF)
        return carry

    t8 = th // 4
    conv(gcat, wt1, 0, th, 0, fin_dx)
    weights(w2v, wc2, False)
    ar_step(2, 3)
    ar_step(0, 2)
    conv(zcat, wc2, 0, t8, 0, fin_y)
    ar_step(1, 2)
    conv(zcat, wc2, t8, th, 0, fin_y)
    for i, n in ((2, 4), (0, 3), (1, 3), (2, 5), (0, 4), (1, 4), (0, 5), (1, 5)):
        ar_step(i, n)


def _flush(n, *refs):
    ins, res, sem = refs[:n], refs[n:2 * n], refs[-1]
    cps = []
    for i in range(n):
        if res[i].shape == ins[i].shape:
            cps.append((ins[i], res[i]))
        else:
            cps += [(ins[i].at[pl.ds((k % 3 * 3 + k // 3) * C, C)], res[i].at[k]) for k in range(NT)]
    cps = [pltpu.make_async_copy(a, b, sem.at[k]) for k, (a, b) in enumerate(cps)]
    for c in cps:
        c.start()
    for c in cps:
        c.wait()


def solution(mesh):
    nh, nw = mesh.shape['h'], mesh.shape['w']
    tile = P(None, 'h', 'w', None)

    def body(x, w1, gamma, beta, w2, g):
        _, th, tw, c = x.shape
        hbm = pl.BlockSpec(memory_space=pltpu.HBM)
        vm = pl.BlockSpec(memory_space=pltpu.VMEM)
        V = pltpu.VMEM
        D = pltpu.SemaphoreType.DMA
        img = jax.ShapeDtypeStruct((th, tw, c), BF)
        wsh = jax.ShapeDtypeStruct((NT * c, c), F32)
        wsp = jax.ShapeDtypeStruct((NT, c, c), F32)
        vec = jax.ShapeDtypeStruct((1, c), F32)
        cat = V((th + 2, tw, 3 * c), BF)
        ndev = nh * nw
        scratch = dict(
            xv=V((th, tw, c), BF), gv=V((th, tw, c), BF),
            wc1=V((12 * c, 2 * c), BF), wt1=V((12 * c, 2 * c), BF), wc2=V((12 * c, 2 * c), BF), wt2=V((12 * c, 2 * c), BF),
            ucat=cat, gcat=cat, zcat=cat, gt=V((th + 4, c, tw), BF), dat=V((th + 4, c, tw), BF),
            av=V((th, tw, c), BF), dn=V((th, tw, c), F32), row=V((tw + TB, c), F32),
            hr=V((3, 2, tw, c), BF), hc=V((3, 2, th, c), F32), hk=V((3, 4, TB, c), BF),
            hrd=V((2, tw, c), F32), hcd=V((2, th, c), F32), hkd=V((4, TB, c), F32), ec=V((4, 2, th, c), F32),
            st=V((2, c), F32), sbuf=V((ndev, 2, c), F32), tt=V((2, c), F32), tbuf=V((ndev, 2, c), F32),
            dwl=V((2, NT * c, c), F32),
            rd=V((3, NT * c // 2, c), F32), rxy=V((3, 3, NT * c // SL, c), F32), zx_buf=V((3, nw, NT * c // SL, c), F32),
            ld=D((2,)), hs=D((4, SL)), hv=D((4, SL)), ss=D((2,)), sr=D((2,)), rs=D((3, 11)), rr=D((3, 11)),
        )
        res = pl.pallas_call(
            functools.partial(_kernel, nh, nw, th, tw),
            out_shape=(img, img, wsh, wsh, vec, vec),
            in_specs=[hbm] * 2 + [vm] * 4,
            out_specs=(vm,) * 6,
            scratch_shapes=list(scratch.values()),
            compiler_params=pltpu.CompilerParams(collective_id=0, has_side_effects=True, vmem_limit_bytes=48 << 20),
        )(x.reshape(th, tw, c), g.reshape(th, tw, c), w1.reshape(NT, c, c), w2.reshape(NT, c, c),
          gamma.reshape(1, c), beta.reshape(1, c))
        y, dx, dw1, dw2, dg, db = pl.pallas_call(
            functools.partial(_flush, len(res)),
            out_shape=(img, img, wsp, wsp, vec, vec),
            in_specs=[vm] * len(res),
            out_specs=(hbm,) * len(res),
            scratch_shapes=[D((4 + 2 * NT,))],
            compiler_params=pltpu.CompilerParams(vmem_limit_bytes=1 << 20),
        )(*res)
        return (y.reshape(x.shape), dx.reshape(x.shape), dw1.reshape(3, 3, c, c), dw2.reshape(3, 3, c, c),
                dg.reshape(c), db.reshape(c))

    return jax.shard_map(body, mesh=mesh, in_specs=(tile, P(), P(), P(), P(), tile),
                         out_specs=(tile, tile, P(), P(), P(), P()), check_vma=False)
```

```python
import functools

import jax
import jax.numpy as jnp
from jax import lax
from jax.experimental import pallas as pl
from jax.experimental.pallas import tpu as pltpu
from jax.sharding import PartitionSpec as P

MESH = pl.DeviceIdType.MESH
GROUPS = 32
EPS = 1e-5
RB, TB, NT, SL = 64, 16, 9, 8
C = 128
C2, C3, ZERO = 2 * C, 3 * C, 0.0
BF = jnp.bfloat16
F32 = jnp.float32
GC = 0.7978845608028654
GC2 = GC * 0.044715
DIRS = ((-1, 0), (1, 0), (0, -1), (0, 1), (-1, -1), (-1, 1), (1, -1), (1, 1))
OPP = (1, 0, 3, 2, 7, 6, 5, 4)


def _group_sum(v):
    lane = lax.broadcasted_iota(jnp.int32, v.shape, 1)
    v = v + jnp.where(lane % 2 == 0, pltpu.roll(v, C - 1, 1), pltpu.roll(v, 1, 1))
    return v + jnp.where(lane % 4 < 2, pltpu.roll(v, C - 2, 1), pltpu.roll(v, 2, 1))


def _fold(v):
    return v.reshape(v.shape[0] // SL, SL, C).sum(0)


def _fold_inner(v):
    it = lax.broadcasted_iota(jnp.int32, (SL, C), 0)
    return _fold(v[SL:-SL]) + jnp.where(it == 0, ZERO, v[:SL]) + jnp.where(it == SL - 1, ZERO, v[-SL:])


def _kernel(nh, nw, th, tw, x_hbm, g_hbm, w12, gb,
            y_ref, dx_ref, dw1_ref, dw2_ref, dgam_ref, dbet_ref,
            xv, gv, wc1, wt1, wc2, wt2, ucat, gcat, zcat, gt, dat, av, dn, row,
            hr, hc, hk, hrd, hcd, hkd, ec,
            st, sbuf, tt, tbuf, dwl, rd, rxy, zx_buf,
            ld, hs, hv, ss, sr, rs, rr):
    w = lax.axis_index('w')
    h = lax.axis_index('h')
    ndev = nh * nw
    me = w * nh + h
    w1v, w2v = w12.at[pl.ds(0, NT)], w12.at[pl.ds(NT, NT)]
    cnt = float(th * nh * tw * nw * (C // GROUPS))

    barrier = pltpu.get_barrier_semaphore()

    def others():
        for dw in range(nw - 1, -1, -1):
            for dh in range(nh - 1, -1, -1):
                if dw or dh:
                    yield lax.rem(w + dw, nw), h ^ dh

    for dev in others():
        pl.semaphore_signal(barrier, inc=1, device_id=dev, device_id_type=MESH)

    loads = [pltpu.make_async_copy(s, d, ld.at[i]) for i, (s, d) in enumerate(
        ((x_hbm, xv), (g_hbm, gv)))]
    for c in loads:
        c.start()

    def neighbour(d):
        dy, dx = DIRS[d]
        hh, ww = h + dy, w + dx
        ok = (hh >= 0) & (hh < nh) & (ww >= 0) & (ww < nw)
        return ok, (ww, hh)

    def bufs(t):
        return (hr.at[t], hc.at[t], hk.at[t]) if t < 3 else (hrd, hcd, hkd)

    def halo(t, rows, start):
        cols = ec.at[t]
        hrow, hcol, hcor = bufs(t)
        for d, (dy, dx) in enumerate(DIRS):
            ok, dev = neighbour(d)
            o = OPP[d]
            r = 0 if dy < 0 else rows.shape[0] - 1
            if dx == 0:
                src, dst = rows.at[r], hrow.at[o]
            elif dy == 0:
                src, dst = cols.at[d - 2], hcol.at[o - 2]
            else:
                src, dst = rows.at[r, pl.ds(0 if dx < 0 else tw - TB, TB)], hcor.at[o - 4]
            cp = pltpu.make_async_remote_copy(src, dst, hs.at[t, d], hv.at[t, o], device_id=dev, device_id_type=MESH)
            if start:
                pl.when(ok)(cp.start)
            else:
                back = pltpu.make_async_remote_copy(
                    src, (hrow.at[d] if dx == 0 else hcol.at[d - 2] if dy == 0 else hcor.at[d - 4]),
                    hs.at[t, d], hv.at[t, d], device_id=dev, device_id_type=MESH)

                @pl.when(ok)
                def _():
                    back.wait_send()
                    back.wait_recv()

    okl = [neighbour(d)[0] for d in range(SL)]

    def first(v):
        return v[0]

    def cat_row(cat, r, shifts=(0, 1, 2)):
        for j in range(0, tw, RB):
            for b in shifts:
                cat[r, pl.ds(j, RB), pl.ds(b * C, C)] = row[pl.ds(SL - 1 + b + j, RB), :].astype(BF)

    def shifted(cat):
        @pl.loop(1, th + 1)
        def _(r):
            for j in range(0, tw, RB):
                row[pl.ds(SL + j, RB), :] = cat[r, pl.ds(j, RB), C:C2].astype(F32)
            cat_row(cat, r, (0, 2))

    def set_ends(left, right):
        row[7:SL, :] = left
        row[tw + SL:tw + NT, :] = right

    def patch(cat, r, left, right):
        it = lax.broadcasted_iota(jnp.int32, (TB, C), 0)
        a = cat[r, 0:TB, 0:C].astype(F32)
        cat[r, 0:TB, 0:C] = jnp.where(it == 0, left, a).astype(BF)
        b = cat[r, tw - TB:tw, C2:C3].astype(F32)
        cat[r, tw - TB:tw, C2:C3] = jnp.where(it == 15, right, b).astype(BF)

    def halo_rows(cat, f, *ts):
        hrow, hcol, hcor = zip(*[bufs(t) for t in ts])
        for e, r in ((0, 0), (1, th + 1)):
            for j in range(0, tw, RB):
                row[pl.ds(SL + j, RB), :] = jnp.where(okl[e], f([b[e, pl.ds(j, RB), :].astype(F32) for b in hrow]), ZERO)
            kl, kr = 2 * e, 2 * e + 1
            cl = f([b[kl].astype(F32) for b in hcor])
            cr = f([b[kr].astype(F32) for b in hcor])
            set_ends(jnp.where(okl[4 + kl], cl[15:TB, :], ZERO), jnp.where(okl[4 + kr], cr[0:1, :], ZERO))
            cat_row(cat, r)

        @pl.loop(0, th // SL)
        def _(k):
            r8 = pl.multiple_of(k * SL, SL)
            lf = jnp.where(okl[2], f([b[0, pl.ds(r8, SL), :].astype(F32) for b in hcol]), ZERO)
            rg = jnp.where(okl[3], f([b[1, pl.ds(r8, SL), :].astype(F32) for b in hcol]), ZERO)
            for i in range(SL):
                patch(cat, r8 + i + 1, lf[i:i + 1, :], rg[i:i + 1, :])

    def build(src, cat, t):
        @pl.loop(0, th)
        def _(r):
            for j in range(0, tw, RB):
                row[pl.ds(SL + j, RB), :] = src[r, pl.ds(j, RB), :].astype(F32)
            ec[t, 0, pl.ds(r, 1), :] = row[SL:NT, :]
            ec[t, 1, pl.ds(r, 1), :] = row[tw + SL - 1:tw + SL, :]
            cat_row(cat, r + 1)

    def weights(wv, wc, flip):
        for r in range(4):
            for b in range(3):
                for t in range(2):
                    k = (r - t) * 3 + b
                    ok = t <= r < t + 3
                    v = jnp.zeros((C, C), BF) if not ok else wv[NT - 1 - k].T if flip else wv[k]
                    wc[pl.ds((r * 3 + b) * C, C), pl.ds(t * C, C)] = v

    def dot(blocks, wc):
        lhs = jnp.concatenate([jnp.concatenate(list(b), axis=1) for b in blocks], axis=0)
        return jnp.dot(lhs, wc[...], preferred_element_type=F32)

    def conv(cat, wc, lo, hi, carry, fn):
        for r0 in range(lo, hi, SL):
            n = min(SL, hi - r0)
            o = dot([[cat[r0 + p + r] for r in range(4)] for p in range(0, n, 2)], wc)
            carry = fn(range(r0, r0 + n), o, carry)
        return carry

    def rows_of(o):
        return [o[(i // 2) * tw:(i // 2 + 1) * tw, (i % 2) * C:(i % 2 + 1) * C] for i in range(2 * o.shape[0] // tw)]

    def wgrad_ab(vt, cat, dst):
        for k in (0, 1, th + 2, th + 3):
            vt[k] = jnp.zeros((C, tw), BF)
        lhs = jnp.concatenate([
            jnp.concatenate([vt[i + 2 - a] for a in range(3)], axis=0) for i in range(th + 2)], axis=1)
        rhs = cat[:, :, pl.ds(0, C2)].reshape((th + 2) * tw, C2)
        o = jnp.dot(lhs, rhs, preferred_element_type=F32)
        for b in range(2):
            for a in range(3):
                dst[pl.ds((b * 3 + a) * C, C), :] = o[a * C:(a + 1) * C, b * C:(b + 1) * C].T

    def wgrad_c(vt, cat, dst):
        n = pl.ds(C2, C)
        rows = range(0, th + 2, 2)
        lhs = jnp.concatenate([jnp.concatenate([vt[i + r] for r in range(4)], axis=0) for i in rows], axis=1)
        rhs = jnp.concatenate([jnp.concatenate([cat[i, :, n], cat[i + 1, :, n]], axis=1) for i in rows], axis=0)
        o = jnp.dot(lhs, rhs, preferred_element_type=F32)
        for a in range(3):
            v = [o[(t + 2 - a) * C:(t + 3 - a) * C, t * C:(t + 1) * C] for t in range(2)]
            dst[pl.ds((6 + a) * C, C), :] = (v[0] + v[1]).T

    def spread(src, buf, i):
        buf[me] = src[...]
        for dev in others():
            pltpu.make_async_remote_copy(src, buf.at[me], ss.at[i], sr.at[i], device_id=dev, device_id_type=MESH).start()

    def gather(buf, i):
        part = buf.at[pl.ds(0, ndev - 1)]
        pltpu.make_async_copy(part, part, sr.at[i]).wait()
        pltpu.make_async_copy(part, part, ss.at[i]).wait()
        s = buf[0]
        for k in range(1, ndev):
            s = s + buf[k]
        return s

    core, q_me = h % 2, h // 2
    jobs = ((0, 0, 6 * C), (0, 6 * C, C3), (1, 0, NT * C))
    outs = (dw1_ref, dw2_ref)

    def ar_step(i, n):
        k_arr, base, rows = jobs[i]
        src, out = dwl.at[k_arr], outs[k_arr]
        half, piece = rows // 2, rows // 8
        buf = pl.ds(0, piece)

        def sl(c, q=0, n=piece):
            return pl.ds(pl.multiple_of(base + c * half + q * piece, SL), n)

        def cp(a, b, k, dev):
            return pltpu.make_async_remote_copy(a, b, rs.at[i, k], rr.at[i, k], device_id=dev, device_id_type=MESH)

        peer = (w, h ^ 1)
        xy = [(k, (w, h ^ (2 * k))) for k in range(1, 4)]
        zp = [(k, lax.rem(w + k, nw), lax.rem(w + nw - k, nw)) for k in range(1, nw)]
        mine = sl(core, q_me)
        pair_rs = cp(src.at[sl(1 - core, 0, half)], rd.at[i, pl.ds(0, half)], 0, peer)
        xy_rs = [cp(src.at[sl(core, q_me ^ k)], rxy.at[i, k - 1, buf], k, dev) for k, dev in xy]
        zx = zx_buf.at[i]
        zx_out = [cp(zx.at[w, buf], zx.at[w, buf], 3 + k, (to, h)) for k, to, _ in zp]
        zx_in = [cp(zx.at[w, buf], zx.at[fr, buf], 3 + k, peer) for k, _, fr in zp]
        xy_out = [cp(out.at[mine], out.at[mine], 6 + k, dev) for k, dev in xy]
        xy_in = [cp(out.at[mine], out.at[sl(core, q_me ^ k)], 6 + k, peer) for k, _ in xy]
        own = out.at[sl(core, 0, half)]
        pair_out = cp(own, own, 10, peer)
        pair_in = cp(own, out.at[sl(1 - core, 0, half)], 10, peer)

        def begin(cps):
            for c in cps:
                c.start()

        def end(sent, got):
            for c in sent:
                c.wait_send()
            for c in got:
                c.wait_recv()

        if n == 0:
            begin([pair_rs])
        elif n == 1:
            end([pair_rs], [pair_rs])
            for k in range(4):
                src[sl(core, k), :] = src[sl(core, k), :] + rd[i, pl.ds(k * piece, piece), :]
            begin(xy_rs)
        elif n == 2:
            end(xy_rs, xy_rs)
            zx[w, buf] = src[mine, :] + rxy[i, 0, buf] + rxy[i, 1, buf] + rxy[i, 2, buf]
            begin(zx_out)
        elif n == 3:
            end(zx_out, zx_in)
            v = zx[0, buf]
            for k in range(1, nw):
                v = v + zx[k, buf]
            out[mine, :] = v
            begin(xy_out)
        elif n == 4:
            end(xy_out, xy_in)
            begin([pair_out])
        else:
            end([pair_out], [pair_in])

    z8 = jnp.zeros((SL, C), F32)
    set_ends(z8[0:1], z8[0:1])
    weights(w1v, wc1, False)
    loads[0].wait()
    build(xv, ucat, 0)

    def fin_a(rows, o, carry):
        s1, s2 = carry
        for r, v in zip(rows, rows_of(o)):
            vb = v.astype(BF)
            av[r] = vb
            vf = vb.astype(F32)
            s1 = s1 + _fold_inner(vf)
            s2 = s2 + _fold_inner(vf * vf)
        return s1, s2

    sums = conv(ucat, wc1, 2, th // 2 + 2, (z8, z8), fin_a)
    pl.semaphore_wait(barrier, ndev - 1)
    halo(0, xv, True)
    sums = conv(ucat, wc1, th // 2 + 2, th - 2, sums, fin_a)

    weights(w2v, wt2, True)
    loads[1].wait()
    build(gv, gcat, 1)
    halo(1, gv, True)

    halo(0, xv, False)
    halo_rows(ucat, first, 0)
    o = dot([[ucat[p + r] for r in range(4)] for p in (0, th - 2)], wc1)
    s1, s2 = fin_a((0, 1, th - 2, th - 1), o, sums)
    it = lax.broadcasted_iota(jnp.int32, (TB, C), 0)
    sides = (pl.ds(0, TB), pl.ds(tw - TB, TB))
    o = dot([[ucat[p + r, s] for r in range(4)] for p in range(0, th, 2) for s in sides], wc1)
    for p in range(th):
        for e, s in enumerate(sides):
            k = (p // 2) * 2 + e
            vb = o[k * TB:(k + 1) * TB, (p % 2) * C:(p % 2 + 1) * C].astype(BF)
            av[p, s] = vb
            vf = jnp.where(it == e * (TB - 1), vb.astype(F32), ZERO)
            ec[2, e, p:p + 1, :] = vf[e * (TB - 1):e * (TB - 1) + 1, :]
            s1 = s1 + _fold(vf)
            s2 = s2 + _fold(vf * vf)
    st[0:1, :] = s1.sum(0, keepdims=True)
    st[1:2, :] = s2.sum(0, keepdims=True)
    spread(st, sbuf, 0)
    halo(2, av, True)

    @pl.loop(0, th)
    def _(r):
        gt[r + 2] = gv[r].T

    halo(1, gv, False)
    halo_rows(gcat, first, 1)

    def fin_dz(rows, o, carry):
        for r, v in zip(rows, rows_of(o)):
            dn[r] = v
        return carry

    conv(gcat, wt2, 0, th, 0, fin_dz)

    tot = _group_sum(gather(sbuf, 0)) / cnt
    mean = tot[0:1, :]
    rstd = lax.rsqrt(tot[1:2, :] - mean * mean + EPS)
    sh = -mean * rstd
    gam, bet = gb[0:1, :], gb[1:2, :]

    def act(a):
        xh = a * rstd + sh
        n = xh * gam + bet
        n2 = n * n
        p = 0.5 + 0.5 * jnp.tanh(n * (GC + GC2 * n2))
        return xh, n2, p, n * p

    def zrow(r, carry):
        t0, t1 = carry
        for j in range(0, tw, RB):
            s = pl.ds(j, RB)
            xh, n2, p, z = act(av[r, s, :].astype(F32))
            zcat[r + 1, s, C:C2] = z.astype(BF)
            d = dn[r, s, :] * (p + z * (1.0 - p) * (2.0 * GC + 6.0 * GC2 * n2))
            dn[r, s, :] = d
            if j == 0:
                ec[3, 0, pl.ds(r, 1), :] = d[0:1, :]
            if j + RB == tw:
                ec[3, 1, pl.ds(r, 1), :] = d[RB - 1:RB, :]
            t0 = t0 + _fold(d * xh)
            t1 = t1 + _fold(d)
        return t0, t1

    t0, t1 = lax.fori_loop(0, th, zrow, (z8, z8))
    tt[0:1, :] = t0.sum(0, keepdims=True)
    tt[1:2, :] = t1.sum(0, keepdims=True)
    spread(tt, tbuf, 1)
    halo(3, dn, True)

    shifted(zcat)
    halo(2, av, False)
    halo_rows(zcat, lambda v: act(v[0])[3], 2)
    wgrad_ab(gt, zcat, dwl.at[1])
    wgrad_c(gt, zcat, dwl.at[1])
    ar_step(2, 0)

    t = gather(tbuf, 1)
    dgam_ref[...] = t[0:1, :]
    dbet_ref[...] = t[1:2, :]
    u = _group_sum(t * gam) / cnt
    k1 = gam * rstd
    k2 = -rstd * rstd * u[0:1, :]
    k3 = -rstd * (u[1:2, :] + sh * u[0:1, :])

    def da_rows(lo, hi):
        @pl.loop(lo, hi)
        def _(r):
            for j in range(0, tw, RB):
                s = pl.ds(j, RB)
                v = (dn[r, s, :] * k1 + av[r, s, :].astype(F32) * k2 + k3).astype(BF)
                gcat[r + 1, s, C:C2] = v
            dat[r + 2] = gcat[r + 1, :, C:C2].T

    da_rows(0, 3 * th // 4)
    ar_step(2, 1)
    da_rows(3 * th // 4, th)

    wgrad_ab(dat, ucat, dwl.at[0])
    ar_step(0, 0)
    wgrad_c(dat, ucat, dwl.at[0])
    ar_step(0, 1)
    ar_step(1, 0)
    weights(w1v, wt1, True)
    ar_step(2, 2)

    shifted(gcat)
    halo(3, dn, False)
    halo_rows(gcat, lambda v: v[0] * k1 + v[1] * k2 + k3, 3, 2)
    ar_step(1, 1)

    def fin_dx(rows, o, carry):
        for r, v in zip(rows, rows_of(o)):
            dx_ref[r] = (v + gv[r].astype(F32)).astype(BF)
        return carry

    def fin_y(rows, o, carry):
        for r, v in zip(rows, rows_of(o)):
            y_ref[r] = (v + xv[r].astype(F32)).astype(BF)
        return carry

    t8 = th // 4
    conv(gcat, wt1, 0, th, 0, fin_dx)
    weights(w2v, wc2, False)
    ar_step(2, 3)
    ar_step(0, 2)
    conv(zcat, wc2, 0, t8, 0, fin_y)
    ar_step(1, 2)
    conv(zcat, wc2, t8, th, 0, fin_y)
    for i, n in ((2, 4), (0, 3), (1, 3), (2, 5), (0, 4), (1, 4), (0, 5), (1, 5)):
        ar_step(i, n)


def _flush(n, *refs):
    ins, res, sem = refs[:n], refs[n:2 * n], refs[-1]
    cps = []
    for i in range(n):
        if res[i].shape == ins[i].shape:
            cps.append((ins[i], res[i]))
        else:
            cps += [(ins[i].at[pl.ds((k % 3 * 3 + k // 3) * C, C)], res[i].at[k]) for k in range(NT)]
    cps = [pltpu.make_async_copy(a, b, sem.at[k]) for k, (a, b) in enumerate(cps)]
    for c in cps:
        c.start()
    for c in cps:
        c.wait()


def solution(mesh):
    nh, nw = mesh.shape['h'], mesh.shape['w']
    tile = P(None, 'h', 'w', None)

    def body(x, w1, gamma, beta, w2, g):
        _, th, tw, c = x.shape
        hbm = pl.BlockSpec(memory_space=pltpu.HBM)
        vm = pl.BlockSpec(memory_space=pltpu.VMEM)
        V = pltpu.VMEM
        D = pltpu.SemaphoreType.DMA
        img = jax.ShapeDtypeStruct((th, tw, c), BF)
        wsh = jax.ShapeDtypeStruct((NT * c, c), F32)
        wsp = jax.ShapeDtypeStruct((NT, c, c), F32)
        vec = jax.ShapeDtypeStruct((1, c), F32)
        cat = V((th + 2, tw, 3 * c), BF)
        ndev = nh * nw
        scratch = dict(
            xv=V((th, tw, c), BF), gv=V((th, tw, c), BF),
            wc1=V((12 * c, 2 * c), BF), wt1=V((12 * c, 2 * c), BF), wc2=V((12 * c, 2 * c), BF), wt2=V((12 * c, 2 * c), BF),
            ucat=cat, gcat=cat, zcat=cat, gt=V((th + 4, c, tw), BF), dat=V((th + 4, c, tw), BF),
            av=V((th, tw, c), BF), dn=V((th, tw, c), F32), row=V((tw + TB, c), F32),
            hr=V((3, 2, tw, c), BF), hc=V((3, 2, th, c), F32), hk=V((3, 4, TB, c), BF),
            hrd=V((2, tw, c), F32), hcd=V((2, th, c), F32), hkd=V((4, TB, c), F32), ec=V((4, 2, th, c), F32),
            st=V((2, c), F32), sbuf=V((ndev, 2, c), F32), tt=V((2, c), F32), tbuf=V((ndev, 2, c), F32),
            dwl=V((2, NT * c, c), F32),
            rd=V((3, NT * c // 2, c), F32), rxy=V((3, 3, NT * c // SL, c), F32), zx_buf=V((3, nw, NT * c // SL, c), F32),
            ld=D((2,)), hs=D((4, SL)), hv=D((4, SL)), ss=D((2,)), sr=D((2,)), rs=D((3, 11)), rr=D((3, 11)),
        )
        res = pl.pallas_call(
            functools.partial(_kernel, nh, nw, th, tw),
            out_shape=(img, img, wsh, wsh, vec, vec),
            in_specs=[hbm] * 2 + [vm] * 2,
            out_specs=(vm,) * 6,
            scratch_shapes=list(scratch.values()),
            compiler_params=pltpu.CompilerParams(collective_id=0, has_side_effects=True, vmem_limit_bytes=48 << 20),
        )(x.reshape(th, tw, c), g.reshape(th, tw, c), jnp.concatenate([w1, w2]).reshape(2 * NT, c, c),
          jnp.stack([gamma, beta]))
        y, dx, dw1, dw2, dg, db = pl.pallas_call(
            functools.partial(_flush, len(res)),
            out_shape=(img, img, wsp, wsp, vec, vec),
            in_specs=[vm] * len(res),
            out_specs=(hbm,) * len(res),
            scratch_shapes=[D((4 + 2 * NT,))],
            compiler_params=pltpu.CompilerParams(vmem_limit_bytes=1 << 20),
        )(*res)
        return (y.reshape(x.shape), dx.reshape(x.shape), dw1.reshape(3, 3, c, c), dw2.reshape(3, 3, c, c),
                dg.reshape(c), db.reshape(c))

    return jax.shard_map(body, mesh=mesh, in_specs=(tile, P(), P(), P(), P(), tile),
                         out_specs=(tile, tile, P(), P(), P(), P()), check_vma=False)
```

```python
import functools

import jax
import jax.numpy as jnp
from jax import lax
from jax.experimental import pallas as pl
from jax.experimental.pallas import tpu as pltpu
from jax.sharding import PartitionSpec as P

MESH = pl.DeviceIdType.MESH
GROUPS = 32
EPS = 1e-5
RB, TB, NT, SL = 64, 16, 9, 8
C = 128
C2, C3, ZERO = 2 * C, 3 * C, 0.0
BF = jnp.bfloat16
F32 = jnp.float32
GC = 0.7978845608028654
GC2 = GC * 0.044715
DIRS = ((-1, 0), (1, 0), (0, -1), (0, 1), (-1, -1), (-1, 1), (1, -1), (1, 1))
OPP = (1, 0, 3, 2, 7, 6, 5, 4)


def _group_sum(v):
    lane = lax.broadcasted_iota(jnp.int32, v.shape, 1)
    v = v + jnp.where(lane % 2 == 0, pltpu.roll(v, C - 1, 1), pltpu.roll(v, 1, 1))
    return v + jnp.where(lane % 4 < 2, pltpu.roll(v, C - 2, 1), pltpu.roll(v, 2, 1))


def _fold(v):
    return v.reshape(v.shape[0] // SL, SL, C).sum(0)


def _fold_inner(v):
    it = lax.broadcasted_iota(jnp.int32, (SL, C), 0)
    return _fold(v[SL:-SL]) + jnp.where(it == 0, ZERO, v[:SL]) + jnp.where(it == SL - 1, ZERO, v[-SL:])


def _kernel(nh, nw, th, tw, x_hbm, g_hbm, w12, gb,
            y_ref, dx_ref, dw1_ref, dw2_ref, dgam_ref, dbet_ref,
            xv, gv, wc1, wt1, wc2, wt2, ucat, gcat, zcat, gt, dat, av, dn, row,
            hr, hc, hk, hrd, hcd, hkd, ec,
            st, sbuf, tt, tbuf, dwl, rd, rxy, zx_buf,
            ld, hs, hv, ss, sr, rs, rr):
    w = lax.axis_index('w')
    h = lax.axis_index('h')
    ndev = nh * nw
    me = w * nh + h
    w1v, w2v = w12.at[pl.ds(0, NT)], w12.at[pl.ds(NT, NT)]
    cnt = float(th * nh * tw * nw * (C // GROUPS))

    barrier = pltpu.get_barrier_semaphore()

    def others():
        for dw in range(nw - 1, -1, -1):
            for dh in range(nh - 1, -1, -1):
                if dw or dh:
                    yield lax.rem(w + dw, nw), h ^ dh

    for dev in others():
        pl.semaphore_signal(barrier, inc=1, device_id=dev, device_id_type=MESH)

    loads = [pltpu.make_async_copy(s, d, ld.at[i]) for i, (s, d) in enumerate(
        ((x_hbm, xv), (g_hbm, gv)))]
    for c in loads:
        c.start()

    def neighbour(d):
        dy, dx = DIRS[d]
        hh, ww = h + dy, w + dx
        ok = (hh >= 0) & (hh < nh) & (ww >= 0) & (ww < nw)
        return ok, (ww, hh)

    def bufs(t):
        return (hr.at[t], hc.at[t], hk.at[t]) if t < 3 else (hrd, hcd, hkd)

    def halo(t, rows, start):
        cols = ec.at[t]
        hrow, hcol, hcor = bufs(t)
        for d, (dy, dx) in enumerate(DIRS):
            ok, dev = neighbour(d)
            o = OPP[d]
            r = 0 if dy < 0 else rows.shape[0] - 1
            if dx == 0:
                src, dst = rows.at[r], hrow.at[o]
            elif dy == 0:
                src, dst = cols.at[d - 2], hcol.at[o - 2]
            else:
                src, dst = rows.at[r, pl.ds(0 if dx < 0 else tw - TB, TB)], hcor.at[o - 4]
            cp = pltpu.make_async_remote_copy(src, dst, hs.at[t, d], hv.at[t, o], device_id=dev, device_id_type=MESH)
            if start:
                pl.when(ok)(cp.start)
            else:
                back = pltpu.make_async_remote_copy(
                    src, (hrow.at[d] if dx == 0 else hcol.at[d - 2] if dy == 0 else hcor.at[d - 4]),
                    hs.at[t, d], hv.at[t, d], device_id=dev, device_id_type=MESH)

                @pl.when(ok)
                def _():
                    back.wait_send()
                    back.wait_recv()

    okl = [neighbour(d)[0] for d in range(SL)]

    def first(v):
        return v[0]

    def cat_row(cat, r, shifts=(0, 1, 2)):
        for j in range(0, tw, RB):
            for b in shifts:
                cat[r, pl.ds(j, RB), pl.ds(b * C, C)] = row[pl.ds(SL - 1 + b + j, RB), :].astype(BF)

    def shifted(cat):
        @pl.loop(1, th + 1)
        def _(r):
            for j in range(0, tw, RB):
                row[pl.ds(SL + j, RB), :] = cat[r, pl.ds(j, RB), C:C2].astype(F32)
            cat_row(cat, r, (0, 2))

    def set_ends(left, right):
        row[7:SL, :] = left
        row[tw + SL:tw + NT, :] = right

    def patch(cat, r, left, right):
        it = lax.broadcasted_iota(jnp.int32, (TB, C), 0)
        a = cat[r, 0:TB, 0:C].astype(F32)
        cat[r, 0:TB, 0:C] = jnp.where(it == 0, left, a).astype(BF)
        b = cat[r, tw - TB:tw, C2:C3].astype(F32)
        cat[r, tw - TB:tw, C2:C3] = jnp.where(it == 15, right, b).astype(BF)

    def halo_rows(cat, f, *ts):
        hrow, hcol, hcor = zip(*[bufs(t) for t in ts])
        for e, r in ((0, 0), (1, th + 1)):
            for j in range(0, tw, RB):
                row[pl.ds(SL + j, RB), :] = jnp.where(okl[e], f([b[e, pl.ds(j, RB), :].astype(F32) for b in hrow]), ZERO)
            kl, kr = 2 * e, 2 * e + 1
            cl = f([b[kl].astype(F32) for b in hcor])
            cr = f([b[kr].astype(F32) for b in hcor])
            set_ends(jnp.where(okl[4 + kl], cl[15:TB, :], ZERO), jnp.where(okl[4 + kr], cr[0:1, :], ZERO))
            cat_row(cat, r)

        @pl.loop(0, th // SL)
        def _(k):
            r8 = pl.multiple_of(k * SL, SL)
            lf = jnp.where(okl[2], f([b[0, pl.ds(r8, SL), :].astype(F32) for b in hcol]), ZERO)
            rg = jnp.where(okl[3], f([b[1, pl.ds(r8, SL), :].astype(F32) for b in hcol]), ZERO)
            for i in range(SL):
                patch(cat, r8 + i + 1, lf[i:i + 1, :], rg[i:i + 1, :])

    def build(src, cat, t):
        @pl.loop(0, th)
        def _(r):
            for j in range(0, tw, RB):
                row[pl.ds(SL + j, RB), :] = src[r, pl.ds(j, RB), :].astype(F32)
            ec[t, 0, pl.ds(r, 1), :] = row[SL:NT, :]
            ec[t, 1, pl.ds(r, 1), :] = row[tw + SL - 1:tw + SL, :]
            cat_row(cat, r + 1)

    def weights(wv, wc, flip):
        for r in range(4):
            for b in range(3):
                for t in range(2):
                    k = (r - t) * 3 + b
                    ok = t <= r < t + 3
                    v = jnp.zeros((C, C), BF) if not ok else wv[NT - 1 - k].T if flip else wv[k]
                    wc[pl.ds((r * 3 + b) * C, C), pl.ds(t * C, C)] = v

    def dot(blocks, wc):
        lhs = jnp.concatenate([jnp.concatenate(list(b), axis=1) for b in blocks], axis=0)
        return jnp.dot(lhs, wc[...], preferred_element_type=F32)

    def conv(cat, wc, lo, hi, carry, fn):
        for r0 in range(lo, hi, SL):
            n = min(SL, hi - r0)
            o = dot([[cat[r0 + p + r] for r in range(4)] for p in range(0, n, 2)], wc)
            carry = fn(range(r0, r0 + n), o, carry)
        return carry

    def rows_of(o):
        return [o[(i // 2) * tw:(i // 2 + 1) * tw, (i % 2) * C:(i % 2 + 1) * C] for i in range(2 * o.shape[0] // tw)]

    def wgrad_ab(vt, cat, dst):
        for k in (0, 1, th + 2, th + 3):
            vt[k] = jnp.zeros((C, tw), BF)
        lhs = jnp.concatenate([
            jnp.concatenate([vt[i + 2 - a] for a in range(3)], axis=0) for i in range(th + 2)], axis=1)
        rhs = cat[:, :, pl.ds(0, C2)].reshape((th + 2) * tw, C2)
        o = jnp.dot(lhs, rhs, preferred_element_type=F32)
        for b in range(2):
            for a in range(3):
                dst[pl.ds((b * 3 + a) * C, C), :] = o[a * C:(a + 1) * C, b * C:(b + 1) * C].T

    def wgrad_c(vt, cat, dst):
        n = pl.ds(C2, C)
        rows = range(0, th + 2, 2)
        lhs = jnp.concatenate([jnp.concatenate([vt[i + r] for r in range(4)], axis=0) for i in rows], axis=1)
        rhs = jnp.concatenate([jnp.concatenate([cat[i, :, n], cat[i + 1, :, n]], axis=1) for i in rows], axis=0)
        o = jnp.dot(lhs, rhs, preferred_element_type=F32)
        for a in range(3):
            v = [o[(t + 2 - a) * C:(t + 3 - a) * C, t * C:(t + 1) * C] for t in range(2)]
            dst[pl.ds((6 + a) * C, C), :] = (v[0] + v[1]).T

    def spread(src, buf, i):
        buf[me] = src[...]
        for dev in others():
            pltpu.make_async_remote_copy(src, buf.at[me], ss.at[i], sr.at[i], device_id=dev, device_id_type=MESH).start()

    def gather(buf, i):
        part = buf.at[pl.ds(0, ndev - 1)]
        pltpu.make_async_copy(part, part, sr.at[i]).wait()
        pltpu.make_async_copy(part, part, ss.at[i]).wait()
        s = buf[0]
        for k in range(1, ndev):
            s = s + buf[k]
        return s

    core, q_me = h % 2, h // 2
    jobs = ((0, 0, NT * C), (1, 0, NT * C))
    outs = (dw1_ref, dw2_ref)

    def ar_step(i, n):
        k_arr, base, rows = jobs[i]
        src, out = dwl.at[k_arr], outs[k_arr]
        half, piece = rows // 2, rows // 8
        buf = pl.ds(0, piece)

        def sl(c, q=0, n=piece):
            return pl.ds(pl.multiple_of(base + c * half + q * piece, SL), n)

        def cp(a, b, k, dev):
            return pltpu.make_async_remote_copy(a, b, rs.at[i, k], rr.at[i, k], device_id=dev, device_id_type=MESH)

        peer = (w, h ^ 1)
        xy = [(k, (w, h ^ (2 * k))) for k in range(1, 4)]
        zp = [(k, lax.rem(w + k, nw), lax.rem(w + nw - k, nw)) for k in range(1, nw)]
        mine = sl(core, q_me)
        pair_rs = cp(src.at[sl(1 - core, 0, half)], rd.at[i, pl.ds(0, half)], 0, peer)
        xy_rs = [cp(src.at[sl(core, q_me ^ k)], rxy.at[i, k - 1, buf], k, dev) for k, dev in xy]
        zx = zx_buf.at[i]
        zx_out = [cp(zx.at[w, buf], zx.at[w, buf], 3 + k, (to, h)) for k, to, _ in zp]
        zx_in = [cp(zx.at[w, buf], zx.at[fr, buf], 3 + k, peer) for k, _, fr in zp]
        xy_out = [cp(out.at[mine], out.at[mine], 6 + k, dev) for k, dev in xy]
        xy_in = [cp(out.at[mine], out.at[sl(core, q_me ^ k)], 6 + k, peer) for k, _ in xy]
        own = out.at[sl(core, 0, half)]
        pair_out = cp(own, own, 10, peer)
        pair_in = cp(own, out.at[sl(1 - core, 0, half)], 10, peer)

        def begin(cps):
            for c in cps:
                c.start()

        def end(sent, got):
            for c in sent:
                c.wait_send()
            for c in got:
                c.wait_recv()

        if n == 0:
            begin([pair_rs])
        elif n == 1:
            end([pair_rs], [pair_rs])
            for k in range(4):
                src[sl(core, k), :] = src[sl(core, k), :] + rd[i, pl.ds(k * piece, piece), :]
            begin(xy_rs)
        elif n == 2:
            end(xy_rs, xy_rs)
            zx[w, buf] = src[mine, :] + rxy[i, 0, buf] + rxy[i, 1, buf] + rxy[i, 2, buf]
            begin(zx_out)
        elif n == 3:
            end(zx_out, zx_in)
            v = zx[0, buf]
            for k in range(1, nw):
                v = v + zx[k, buf]
            out[mine, :] = v
            begin(xy_out)
        elif n == 4:
            end(xy_out, xy_in)
            begin([pair_out])
        else:
            end([pair_out], [pair_in])

    z8 = jnp.zeros((SL, C), F32)
    set_ends(z8[0:1], z8[0:1])
    weights(w1v, wc1, False)
    loads[0].wait()
    build(xv, ucat, 0)

    def fin_a(rows, o, carry):
        s1, s2 = carry
        for r, v in zip(rows, rows_of(o)):
            vb = v.astype(BF)
            av[r] = vb
            vf = vb.astype(F32)
            s1 = s1 + _fold_inner(vf)
            s2 = s2 + _fold_inner(vf * vf)
        return s1, s2

    sums = conv(ucat, wc1, 2, th // 2 + 2, (z8, z8), fin_a)
    pl.semaphore_wait(barrier, ndev - 1)
    halo(0, xv, True)
    sums = conv(ucat, wc1, th // 2 + 2, th - 2, sums, fin_a)

    weights(w2v, wt2, True)
    loads[1].wait()
    build(gv, gcat, 1)
    halo(1, gv, True)

    halo(0, xv, False)
    halo_rows(ucat, first, 0)
    o = dot([[ucat[p + r] for r in range(4)] for p in (0, th - 2)], wc1)
    s1, s2 = fin_a((0, 1, th - 2, th - 1), o, sums)
    it = lax.broadcasted_iota(jnp.int32, (TB, C), 0)
    sides = (pl.ds(0, TB), pl.ds(tw - TB, TB))
    o = dot([[ucat[p + r, s] for r in range(4)] for p in range(0, th, 2) for s in sides], wc1)
    for p in range(th):
        for e, s in enumerate(sides):
            k = (p // 2) * 2 + e
            vb = o[k * TB:(k + 1) * TB, (p % 2) * C:(p % 2 + 1) * C].astype(BF)
            av[p, s] = vb
            vf = jnp.where(it == e * (TB - 1), vb.astype(F32), ZERO)
            ec[2, e, p:p + 1, :] = vf[e * (TB - 1):e * (TB - 1) + 1, :]
            s1 = s1 + _fold(vf)
            s2 = s2 + _fold(vf * vf)
    st[0:1, :] = s1.sum(0, keepdims=True)
    st[1:2, :] = s2.sum(0, keepdims=True)
    spread(st, sbuf, 0)
    halo(2, av, True)

    @pl.loop(0, th)
    def _(r):
        gt[r + 2] = gv[r].T

    halo(1, gv, False)
    halo_rows(gcat, first, 1)

    def fin_dz(rows, o, carry):
        for r, v in zip(rows, rows_of(o)):
            dn[r] = v
        return carry

    conv(gcat, wt2, 0, th, 0, fin_dz)

    tot = _group_sum(gather(sbuf, 0)) / cnt
    mean = tot[0:1, :]
    rstd = lax.rsqrt(tot[1:2, :] - mean * mean + EPS)
    sh = -mean * rstd
    gam, bet = gb[0:1, :], gb[1:2, :]

    def act(a):
        xh = a * rstd + sh
        n = xh * gam + bet
        n2 = n * n
        p = 0.5 + 0.5 * jnp.tanh(n * (GC + GC2 * n2))
        return xh, n2, p, n * p

    def zrow(r, carry):
        t0, t1 = carry
        for j in range(0, tw, RB):
            s = pl.ds(j, RB)
            xh, n2, p, z = act(av[r, s, :].astype(F32))
            zcat[r + 1, s, C:C2] = z.astype(BF)
            d = dn[r, s, :] * (p + z * (1.0 - p) * (2.0 * GC + 6.0 * GC2 * n2))
            dn[r, s, :] = d
            if j == 0:
                ec[3, 0, pl.ds(r, 1), :] = d[0:1, :]
            if j + RB == tw:
                ec[3, 1, pl.ds(r, 1), :] = d[RB - 1:RB, :]
            t0 = t0 + _fold(d * xh)
            t1 = t1 + _fold(d)
        return t0, t1

    t0, t1 = lax.fori_loop(0, th, zrow, (z8, z8))
    tt[0:1, :] = t0.sum(0, keepdims=True)
    tt[1:2, :] = t1.sum(0, keepdims=True)
    spread(tt, tbuf, 1)
    halo(3, dn, True)

    shifted(zcat)
    halo(2, av, False)
    halo_rows(zcat, lambda v: act(v[0])[3], 2)
    wgrad_ab(gt, zcat, dwl.at[1])
    wgrad_c(gt, zcat, dwl.at[1])
    ar_step(1, 0)

    t = gather(tbuf, 1)
    dgam_ref[...] = t[0:1, :]
    dbet_ref[...] = t[1:2, :]
    u = _group_sum(t * gam) / cnt
    k1 = gam * rstd
    k2 = -rstd * rstd * u[0:1, :]
    k3 = -rstd * (u[1:2, :] + sh * u[0:1, :])

    def da_rows(lo, hi):
        @pl.loop(lo, hi)
        def _(r):
            for j in range(0, tw, RB):
                s = pl.ds(j, RB)
                v = (dn[r, s, :] * k1 + av[r, s, :].astype(F32) * k2 + k3).astype(BF)
                gcat[r + 1, s, C:C2] = v
            dat[r + 2] = gcat[r + 1, :, C:C2].T

    da_rows(0, 3 * th // 4)
    ar_step(1, 1)
    da_rows(3 * th // 4, th)

    wgrad_ab(dat, ucat, dwl.at[0])
    wgrad_c(dat, ucat, dwl.at[0])
    ar_step(0, 0)
    weights(w1v, wt1, True)
    ar_step(0, 1)
    ar_step(1, 2)

    shifted(gcat)
    halo(3, dn, False)
    halo_rows(gcat, lambda v: v[0] * k1 + v[1] * k2 + k3, 3, 2)

    def fin_dx(rows, o, carry):
        for r, v in zip(rows, rows_of(o)):
            dx_ref[r] = (v + gv[r].astype(F32)).astype(BF)
        return carry

    def fin_y(rows, o, carry):
        for r, v in zip(rows, rows_of(o)):
            y_ref[r] = (v + xv[r].astype(F32)).astype(BF)
        return carry

    conv(gcat, wt1, 0, th, 0, fin_dx)
    weights(w2v, wc2, False)
    ar_step(1, 3)
    ar_step(0, 2)
    conv(zcat, wc2, 0, th, 0, fin_y)
    for i, n in ((1, 4), (0, 3), (1, 5), (0, 4), (0, 5)):
        ar_step(i, n)


def _flush(n, *refs):
    ins, res, sem = refs[:n], refs[n:2 * n], refs[-1]
    cps = []
    for i in range(n):
        if res[i].shape == ins[i].shape:
            cps.append((ins[i], res[i]))
        else:
            cps += [(ins[i].at[pl.ds((k % 3 * 3 + k // 3) * C, C)], res[i].at[k]) for k in range(NT)]
    cps = [pltpu.make_async_copy(a, b, sem.at[k]) for k, (a, b) in enumerate(cps)]
    for c in cps:
        c.start()
    for c in cps:
        c.wait()


def solution(mesh):
    nh, nw = mesh.shape['h'], mesh.shape['w']
    tile = P(None, 'h', 'w', None)

    def body(x, w1, gamma, beta, w2, g):
        _, th, tw, c = x.shape
        hbm = pl.BlockSpec(memory_space=pltpu.HBM)
        vm = pl.BlockSpec(memory_space=pltpu.VMEM)
        V = pltpu.VMEM
        D = pltpu.SemaphoreType.DMA
        img = jax.ShapeDtypeStruct((th, tw, c), BF)
        wsh = jax.ShapeDtypeStruct((NT * c, c), F32)
        wsp = jax.ShapeDtypeStruct((NT, c, c), F32)
        vec = jax.ShapeDtypeStruct((1, c), F32)
        cat = V((th + 2, tw, 3 * c), BF)
        ndev = nh * nw
        scratch = dict(
            xv=V((th, tw, c), BF), gv=V((th, tw, c), BF),
            wc1=V((12 * c, 2 * c), BF), wt1=V((12 * c, 2 * c), BF), wc2=V((12 * c, 2 * c), BF), wt2=V((12 * c, 2 * c), BF),
            ucat=cat, gcat=cat, zcat=cat, gt=V((th + 4, c, tw), BF), dat=V((th + 4, c, tw), BF),
            av=V((th, tw, c), BF), dn=V((th, tw, c), F32), row=V((tw + TB, c), F32),
            hr=V((3, 2, tw, c), BF), hc=V((3, 2, th, c), F32), hk=V((3, 4, TB, c), BF),
            hrd=V((2, tw, c), F32), hcd=V((2, th, c), F32), hkd=V((4, TB, c), F32), ec=V((4, 2, th, c), F32),
            st=V((2, c), F32), sbuf=V((ndev, 2, c), F32), tt=V((2, c), F32), tbuf=V((ndev, 2, c), F32),
            dwl=V((2, NT * c, c), F32),
            rd=V((2, NT * c // 2, c), F32), rxy=V((2, 3, NT * c // SL, c), F32), zx_buf=V((2, nw, NT * c // SL, c), F32),
            ld=D((2,)), hs=D((4, SL)), hv=D((4, SL)), ss=D((2,)), sr=D((2,)), rs=D((2, 11)), rr=D((2, 11)),
        )
        res = pl.pallas_call(
            functools.partial(_kernel, nh, nw, th, tw),
            out_shape=(img, img, wsh, wsh, vec, vec),
            in_specs=[hbm] * 2 + [vm] * 2,
            out_specs=(vm,) * 6,
            scratch_shapes=list(scratch.values()),
            compiler_params=pltpu.CompilerParams(collective_id=0, has_side_effects=True, vmem_limit_bytes=48 << 20),
        )(x.reshape(th, tw, c), g.reshape(th, tw, c), jnp.concatenate([w1, w2]).reshape(2 * NT, c, c),
          jnp.stack([gamma, beta]))
        y, dx, dw1, dw2, dg, db = pl.pallas_call(
            functools.partial(_flush, len(res)),
            out_shape=(img, img, wsp, wsp, vec, vec),
            in_specs=[vm] * len(res),
            out_specs=(hbm,) * len(res),
            scratch_shapes=[D((4 + 2 * NT,))],
            compiler_params=pltpu.CompilerParams(vmem_limit_bytes=1 << 20),
        )(*res)
        return (y.reshape(x.shape), dx.reshape(x.shape), dw1.reshape(3, 3, c, c), dw2.reshape(3, 3, c, c),
                dg.reshape(c), db.reshape(c))

    return jax.shard_map(body, mesh=mesh, in_specs=(tile, P(), P(), P(), P(), tile),
                         out_specs=(tile, tile, P(), P(), P(), P()), check_vma=False)
```

```python
import functools

import jax
import jax.numpy as jnp
from jax import lax
from jax.experimental import pallas as pl
from jax.experimental.pallas import tpu as pltpu
from jax.sharding import PartitionSpec as P

MESH = pl.DeviceIdType.MESH
GROUPS = 32
EPS = 1e-5
RB, TB, NT, SL = 64, 16, 9, 8
C = 128
C2, C3, ZERO = 2 * C, 3 * C, 0.0
BF = jnp.bfloat16
F32 = jnp.float32
GC = 0.7978845608028654
GC2 = GC * 0.044715
DIRS = ((-1, 0), (1, 0), (0, -1), (0, 1), (-1, -1), (-1, 1), (1, -1), (1, 1))
OPP = (1, 0, 3, 2, 7, 6, 5, 4)


def _group_sum(v):
    lane = lax.broadcasted_iota(jnp.int32, v.shape, 1)
    v = v + jnp.where(lane % 2 == 0, pltpu.roll(v, C - 1, 1), pltpu.roll(v, 1, 1))
    return v + jnp.where(lane % 4 < 2, pltpu.roll(v, C - 2, 1), pltpu.roll(v, 2, 1))


def _fold(v):
    return v.reshape(v.shape[0] // SL, SL, C).sum(0)


def _fold_inner(v):
    it = lax.broadcasted_iota(jnp.int32, (SL, C), 0)
    return _fold(v[SL:-SL]) + jnp.where(it == 0, ZERO, v[:SL]) + jnp.where(it == SL - 1, ZERO, v[-SL:])


def _kernel(nh, nw, th, tw, x_hbm, g_hbm, w12, gb,
            y_ref, dx_ref, dw1_ref, dw2_ref, dgam_ref, dbet_ref,
            xv, gv, wc1, wt1, wc2, wt2, ucat, gcat, zcat, gt, dat, av, dn, row,
            hr, hc, hk, hrd, hcd, hkd, ec,
            st, sbuf, tt, tbuf, dwl, rd, rxy, zx_buf,
            ld, hs, hv, ss, sr, rs, rr):
    w = lax.axis_index('w')
    h = lax.axis_index('h')
    ndev = nh * nw
    me = w * nh + h
    w1v, w2v = w12.at[pl.ds(0, NT)], w12.at[pl.ds(NT, NT)]
    cnt = float(th * nh * tw * nw * (C // GROUPS))

    barrier = pltpu.get_barrier_semaphore()

    def others():
        for dw in range(nw - 1, -1, -1):
            for dh in range(nh - 1, -1, -1):
                if dw or dh:
                    yield lax.rem(w + dw, nw), h ^ dh

    for dev in others():
        pl.semaphore_signal(barrier, inc=1, device_id=dev, device_id_type=MESH)

    loads = [pltpu.make_async_copy(s, d, ld.at[i]) for i, (s, d) in enumerate(
        ((x_hbm, xv), (g_hbm, gv)))]
    for c in loads:
        c.start()

    def neighbour(d):
        dy, dx = DIRS[d]
        hh, ww = h + dy, w + dx
        ok = (hh >= 0) & (hh < nh) & (ww >= 0) & (ww < nw)
        return ok, (ww, hh)

    def bufs(t):
        return (hr.at[t], hc.at[t], hk.at[t]) if t < 3 else (hrd, hcd, hkd)

    def halo(t, rows, start):
        cols = ec.at[t]
        hrow, hcol, hcor = bufs(t)
        for d, (dy, dx) in enumerate(DIRS):
            ok, dev = neighbour(d)
            o = OPP[d]
            r = 0 if dy < 0 else rows.shape[0] - 1
            if dx == 0:
                src, dst = rows.at[r], hrow.at[o]
            elif dy == 0:
                src, dst = cols.at[d - 2], hcol.at[o - 2]
            else:
                src, dst = rows.at[r, pl.ds(0 if dx < 0 else tw - TB, TB)], hcor.at[o - 4]
            cp = pltpu.make_async_remote_copy(src, dst, hs.at[t, d], hv.at[t, o], device_id=dev, device_id_type=MESH)
            if start:
                pl.when(ok)(cp.start)
            else:
                back = pltpu.make_async_remote_copy(
                    src, (hrow.at[d] if dx == 0 else hcol.at[d - 2] if dy == 0 else hcor.at[d - 4]),
                    hs.at[t, d], hv.at[t, d], device_id=dev, device_id_type=MESH)

                @pl.when(ok)
                def _():
                    back.wait_send()
                    back.wait_recv()

    okl = [neighbour(d)[0] for d in range(SL)]

    def first(v):
        return v[0]

    def cat_row(cat, r, shifts=(0, 1, 2)):
        for j in range(0, tw, RB):
            for b in shifts:
                cat[r, pl.ds(j, RB), pl.ds(b * C, C)] = row[pl.ds(SL - 1 + b + j, RB), :].astype(BF)

    def shifted(cat):
        @pl.loop(1, th + 1)
        def _(r):
            for j in range(0, tw, RB):
                row[pl.ds(SL + j, RB), :] = cat[r, pl.ds(j, RB), C:C2].astype(F32)
            cat_row(cat, r, (0, 2))

    def set_ends(left, right):
        row[7:SL, :] = left
        row[tw + SL:tw + NT, :] = right

    def patch(cat, r, left, right):
        it = lax.broadcasted_iota(jnp.int32, (TB, C), 0)
        a = cat[r, 0:TB, 0:C].astype(F32)
        cat[r, 0:TB, 0:C] = jnp.where(it == 0, left, a).astype(BF)
        b = cat[r, tw - TB:tw, C2:C3].astype(F32)
        cat[r, tw - TB:tw, C2:C3] = jnp.where(it == 15, right, b).astype(BF)

    def halo_rows(cat, f, *ts):
        hrow, hcol, hcor = zip(*[bufs(t) for t in ts])
        for e, r in ((0, 0), (1, th + 1)):
            for j in range(0, tw, RB):
                row[pl.ds(SL + j, RB), :] = jnp.where(okl[e], f([b[e, pl.ds(j, RB), :].astype(F32) for b in hrow]), ZERO)
            kl, kr = 2 * e, 2 * e + 1
            cl = f([b[kl].astype(F32) for b in hcor])
            cr = f([b[kr].astype(F32) for b in hcor])
            set_ends(jnp.where(okl[4 + kl], cl[15:TB, :], ZERO), jnp.where(okl[4 + kr], cr[0:1, :], ZERO))
            cat_row(cat, r)

        @pl.loop(0, th // SL)
        def _(k):
            r8 = pl.multiple_of(k * SL, SL)
            lf = jnp.where(okl[2], f([b[0, pl.ds(r8, SL), :].astype(F32) for b in hcol]), ZERO)
            rg = jnp.where(okl[3], f([b[1, pl.ds(r8, SL), :].astype(F32) for b in hcol]), ZERO)
            for i in range(SL):
                patch(cat, r8 + i + 1, lf[i:i + 1, :], rg[i:i + 1, :])

    def build(src, cat, t):
        @pl.loop(0, th)
        def _(r):
            for j in range(0, tw, RB):
                row[pl.ds(SL + j, RB), :] = src[r, pl.ds(j, RB), :].astype(F32)
            ec[t, 0, pl.ds(r, 1), :] = row[SL:NT, :]
            ec[t, 1, pl.ds(r, 1), :] = row[tw + SL - 1:tw + SL, :]
            cat_row(cat, r + 1)

    def weights(wv, wc, flip):
        for r in range(4):
            for b in range(3):
                for t in range(2):
                    k = (r - t) * 3 + b
                    ok = t <= r < t + 3
                    v = jnp.zeros((C, C), BF) if not ok else wv[NT - 1 - k].T if flip else wv[k]
                    wc[pl.ds((r * 3 + b) * C, C), pl.ds(t * C, C)] = v

    def dot(blocks, wc):
        lhs = jnp.concatenate([jnp.concatenate(list(b), axis=1) for b in blocks], axis=0)
        return jnp.dot(lhs, wc[...], preferred_element_type=F32)

    def conv(cat, wc, lo, hi, carry, fn):
        for r0 in range(lo, hi, SL):
            n = min(SL, hi - r0)
            o = dot([[cat[r0 + p + r] for r in range(4)] for p in range(0, n, 2)], wc)
            carry = fn(range(r0, r0 + n), o, carry)
        return carry

    def rows_of(o):
        return [o[(i // 2) * tw:(i // 2 + 1) * tw, (i % 2) * C:(i % 2 + 1) * C] for i in range(2 * o.shape[0] // tw)]

    def wgrad_ab(vt, cat, dst):
        for k in (0, 1, th + 2, th + 3):
            vt[k] = jnp.zeros((C, tw), BF)
        lhs = jnp.concatenate([
            jnp.concatenate([vt[i + 2 - a] for a in range(3)], axis=0) for i in range(th + 2)], axis=1)
        rhs = cat[:, :, pl.ds(0, C2)].reshape((th + 2) * tw, C2)
        o = jnp.dot(lhs, rhs, preferred_element_type=F32)
        for b in range(2):
            for a in range(3):
                dst[pl.ds((b * 3 + a) * C, C), :] = o[a * C:(a + 1) * C, b * C:(b + 1) * C].T

    def wgrad_c(vt, cat, dst):
        n = pl.ds(C2, C)
        rows = range(0, th + 2, 2)
        lhs = jnp.concatenate([jnp.concatenate([vt[i + r] for r in range(4)], axis=0) for i in rows], axis=1)
        rhs = jnp.concatenate([jnp.concatenate([cat[i, :, n], cat[i + 1, :, n]], axis=1) for i in rows], axis=0)
        o = jnp.dot(lhs, rhs, preferred_element_type=F32)
        for a in range(3):
            v = [o[(t + 2 - a) * C:(t + 3 - a) * C, t * C:(t + 1) * C] for t in range(2)]
            dst[pl.ds((6 + a) * C, C), :] = (v[0] + v[1]).T

    def spread(src, buf, i):
        buf[me] = src[...]
        for dev in others():
            pltpu.make_async_remote_copy(src, buf.at[me], ss.at[i], sr.at[i], device_id=dev, device_id_type=MESH).start()

    def gather(buf, i):
        part = buf.at[pl.ds(0, ndev - 1)]
        pltpu.make_async_copy(part, part, sr.at[i]).wait()
        pltpu.make_async_copy(part, part, ss.at[i]).wait()
        s = buf[0]
        for k in range(1, ndev):
            s = s + buf[k]
        return s

    core, q_me = h % 2, h // 2
    jobs = ((0, 0, NT * C), (1, 0, NT * C))
    outs = (dw1_ref, dw2_ref)

    def ar_step(i, n):
        k_arr, base, rows = jobs[i]
        src, out = dwl.at[k_arr], outs[k_arr]
        half, piece = rows // 2, rows // 8
        buf = pl.ds(0, piece)

        def sl(c, q=0, n=piece):
            return pl.ds(pl.multiple_of(base + c * half + q * piece, SL), n)

        def cp(a, b, k, dev):
            return pltpu.make_async_remote_copy(a, b, rs.at[i, k], rr.at[i, k], device_id=dev, device_id_type=MESH)

        peer = (w, h ^ 1)
        xy = [(k, (w, h ^ (2 * k))) for k in range(1, 4)]
        zp = [(k, lax.rem(w + k, nw), lax.rem(w + nw - k, nw)) for k in range(1, nw)]
        mine = sl(core, q_me)
        pair_rs = cp(src.at[sl(1 - core, 0, half)], rd.at[i, pl.ds(0, half)], 0, peer)
        xy_rs = [cp(src.at[sl(core, q_me ^ k)], rxy.at[i, k - 1, buf], k, dev) for k, dev in xy]
        zx = zx_buf.at[i]
        zx_out = [cp(zx.at[w, buf], zx.at[w, buf], 3 + k, (to, h)) for k, to, _ in zp]
        zx_in = [cp(zx.at[w, buf], zx.at[fr, buf], 3 + k, peer) for k, _, fr in zp]
        xy_out = [cp(out.at[mine], out.at[mine], 6 + k, dev) for k, dev in xy]
        xy_in = [cp(out.at[mine], out.at[sl(core, q_me ^ k)], 6 + k, peer) for k, _ in xy]
        own = out.at[sl(core, 0, half)]
        pair_out = cp(own, own, 10, peer)
        pair_in = cp(own, out.at[sl(1 - core, 0, half)], 10, peer)

        def begin(cps):
            for c in cps:
                c.start()

        def end(sent, got):
            for c in sent:
                c.wait_send()
            for c in got:
                c.wait_recv()

        if n == 0:
            begin([pair_rs])
        elif n == 1:
            end([pair_rs], [pair_rs])
            for k in range(4):
                src[sl(core, k), :] = src[sl(core, k), :] + rd[i, pl.ds(k * piece, piece), :]
            begin(xy_rs)
        elif n == 2:
            end(xy_rs, xy_rs)
            zx[w, buf] = src[mine, :] + rxy[i, 0, buf] + rxy[i, 1, buf] + rxy[i, 2, buf]
            begin(zx_out)
        elif n == 3:
            end(zx_out, zx_in)
            v = zx[0, buf]
            for k in range(1, nw):
                v = v + zx[k, buf]
            out[mine, :] = v
            begin(xy_out)
        elif n == 4:
            end(xy_out, xy_in)
            begin([pair_out])
        else:
            end([pair_out], [pair_in])

    z8 = jnp.zeros((SL, C), F32)
    set_ends(z8[0:1], z8[0:1])
    weights(w1v, wc1, False)
    loads[0].wait()
    build(xv, ucat, 0)

    def fin_a(rows, o, carry):
        s1, s2 = carry
        for r, v in zip(rows, rows_of(o)):
            vb = v.astype(BF)
            av[r] = vb
            vf = vb.astype(F32)
            s1 = s1 + _fold_inner(vf)
            s2 = s2 + _fold_inner(vf * vf)
        return s1, s2

    sums = conv(ucat, wc1, 2, th // 2 + 2, (z8, z8), fin_a)
    pl.semaphore_wait(barrier, ndev - 1)
    halo(0, xv, True)
    sums = conv(ucat, wc1, th // 2 + 2, th - 2, sums, fin_a)

    weights(w2v, wt2, True)
    loads[1].wait()
    build(gv, gcat, 1)
    halo(1, gv, True)

    halo(0, xv, False)
    halo_rows(ucat, first, 0)
    o = dot([[ucat[p + r] for r in range(4)] for p in (0, th - 2)], wc1)
    s1, s2 = fin_a((0, 1, th - 2, th - 1), o, sums)
    it = lax.broadcasted_iota(jnp.int32, (TB, C), 0)
    sides = (pl.ds(0, TB), pl.ds(tw - TB, TB))
    o = dot([[ucat[p + r, s] for r in range(4)] for p in range(0, th, 2) for s in sides], wc1)
    for p in range(th):
        for e, s in enumerate(sides):
            k = (p // 2) * 2 + e
            vb = o[k * TB:(k + 1) * TB, (p % 2) * C:(p % 2 + 1) * C].astype(BF)
            av[p, s] = vb
            vf = jnp.where(it == e * (TB - 1), vb.astype(F32), ZERO)
            ec[2, e, p:p + 1, :] = vf[e * (TB - 1):e * (TB - 1) + 1, :]
            s1 = s1 + _fold(vf)
            s2 = s2 + _fold(vf * vf)
    st[0:1, :] = s1.sum(0, keepdims=True)
    st[1:2, :] = s2.sum(0, keepdims=True)
    spread(st, sbuf, 0)
    halo(2, av, True)

    @pl.loop(0, th)
    def _(r):
        gt[r + 2] = gv[r].T

    halo(1, gv, False)
    halo_rows(gcat, first, 1)

    def fin_dz(rows, o, carry):
        for r, v in zip(rows, rows_of(o)):
            dn[r] = v
        return carry

    conv(gcat, wt2, 0, th, 0, fin_dz)

    tot = _group_sum(gather(sbuf, 0)) / cnt
    mean = tot[0:1, :]
    rstd = lax.rsqrt(tot[1:2, :] - mean * mean + EPS)
    sh = -mean * rstd
    gam, bet = gb[0:1, :], gb[1:2, :]

    def act(a):
        xh = a * rstd + sh
        n = xh * gam + bet
        n2 = n * n
        p = 0.5 + 0.5 * jnp.tanh(n * (GC + GC2 * n2))
        return xh, n2, p, n * p

    def zrow(r, carry):
        t0, t1 = carry
        for j in range(0, tw, RB):
            s = pl.ds(j, RB)
            xh, n2, p, z = act(av[r, s, :].astype(F32))
            zcat[r + 1, s, C:C2] = z.astype(BF)
            d = dn[r, s, :] * (p + z * (1.0 - p) * (2.0 * GC + 6.0 * GC2 * n2))
            dn[r, s, :] = d
            if j == 0:
                ec[3, 0, pl.ds(r, 1), :] = d[0:1, :]
            if j + RB == tw:
                ec[3, 1, pl.ds(r, 1), :] = d[RB - 1:RB, :]
            t0 = t0 + _fold(d * xh)
            t1 = t1 + _fold(d)
        return t0, t1

    t0, t1 = lax.fori_loop(0, th, zrow, (z8, z8))
    tt[0:1, :] = t0.sum(0, keepdims=True)
    tt[1:2, :] = t1.sum(0, keepdims=True)
    spread(tt, tbuf, 1)
    halo(3, dn, True)

    shifted(zcat)
    halo(2, av, False)
    halo_rows(zcat, lambda v: act(v[0])[3], 2)
    wgrad_ab(gt, zcat, dwl.at[1])
    wgrad_c(gt, zcat, dwl.at[1])
    ar_step(1, 0)

    t = gather(tbuf, 1)
    dgam_ref[...] = t[0:1, :]
    dbet_ref[...] = t[1:2, :]
    u = _group_sum(t * gam) / cnt
    k1 = gam * rstd
    k2 = -rstd * rstd * u[0:1, :]
    k3 = -rstd * (u[1:2, :] + sh * u[0:1, :])

    def da_rows(lo, hi):
        @pl.loop(lo, hi)
        def _(r):
            for j in range(0, tw, RB):
                s = pl.ds(j, RB)
                v = (dn[r, s, :] * k1 + av[r, s, :].astype(F32) * k2 + k3).astype(BF)
                gcat[r + 1, s, C:C2] = v
            dat[r + 2] = gcat[r + 1, :, C:C2].T

    da_rows(0, 3 * th // 4)
    ar_step(1, 1)
    da_rows(3 * th // 4, th)

    wgrad_ab(dat, ucat, dwl.at[0])
    wgrad_c(dat, ucat, dwl.at[0])
    ar_step(0, 0)
    weights(w1v, wt1, True)
    ar_step(0, 1)
    ar_step(1, 2)

    shifted(gcat)
    halo(3, dn, False)
    halo_rows(gcat, lambda v: v[0] * k1 + v[1] * k2 + k3, 3, 2)

    def fin_dx(rows, o, carry):
        for r, v in zip(rows, rows_of(o)):
            dx_ref[r] = (v + gv[r].astype(F32)).astype(BF)
        return carry

    def fin_y(rows, o, carry):
        for r, v in zip(rows, rows_of(o)):
            y_ref[r] = (v + xv[r].astype(F32)).astype(BF)
        return carry

    conv(gcat, wt1, 0, th, 0, fin_dx)
    weights(w2v, wc2, False)
    ar_step(0, 2)
    ar_step(1, 3)
    conv(zcat, wc2, 0, th, 0, fin_y)
    for i, n in ((1, 4), (0, 3), (1, 5), (0, 4), (0, 5)):
        ar_step(i, n)


def _flush(n, *refs):
    ins, res, sem = refs[:n], refs[n:2 * n], refs[-1]
    cps = []
    for i in range(n):
        if res[i].shape == ins[i].shape:
            cps.append((ins[i], res[i]))
        else:
            cps += [(ins[i].at[pl.ds((k % 3 * 3 + k // 3) * C, C)], res[i].at[k]) for k in range(NT)]
    cps = [pltpu.make_async_copy(a, b, sem.at[k]) for k, (a, b) in enumerate(cps)]
    for c in cps:
        c.start()
    for c in cps:
        c.wait()


def solution(mesh):
    nh, nw = mesh.shape['h'], mesh.shape['w']
    tile = P(None, 'h', 'w', None)

    def body(x, w1, gamma, beta, w2, g):
        _, th, tw, c = x.shape
        hbm = pl.BlockSpec(memory_space=pltpu.HBM)
        vm = pl.BlockSpec(memory_space=pltpu.VMEM)
        V = pltpu.VMEM
        D = pltpu.SemaphoreType.DMA
        img = jax.ShapeDtypeStruct((th, tw, c), BF)
        wsh = jax.ShapeDtypeStruct((NT * c, c), F32)
        wsp = jax.ShapeDtypeStruct((NT, c, c), F32)
        vec = jax.ShapeDtypeStruct((1, c), F32)
        cat = V((th + 2, tw, 3 * c), BF)
        ndev = nh * nw
        scratch = dict(
            xv=V((th, tw, c), BF), gv=V((th, tw, c), BF),
            wc1=V((12 * c, 2 * c), BF), wt1=V((12 * c, 2 * c), BF), wc2=V((12 * c, 2 * c), BF), wt2=V((12 * c, 2 * c), BF),
            ucat=cat, gcat=cat, zcat=cat, gt=V((th + 4, c, tw), BF), dat=V((th + 4, c, tw), BF),
            av=V((th, tw, c), BF), dn=V((th, tw, c), F32), row=V((tw + TB, c), F32),
            hr=V((3, 2, tw, c), BF), hc=V((3, 2, th, c), F32), hk=V((3, 4, TB, c), BF),
            hrd=V((2, tw, c), F32), hcd=V((2, th, c), F32), hkd=V((4, TB, c), F32), ec=V((4, 2, th, c), F32),
            st=V((2, c), F32), sbuf=V((ndev, 2, c), F32), tt=V((2, c), F32), tbuf=V((ndev, 2, c), F32),
            dwl=V((2, NT * c, c), F32),
            rd=V((2, NT * c // 2, c), F32), rxy=V((2, 3, NT * c // SL, c), F32), zx_buf=V((2, nw, NT * c // SL, c), F32),
            ld=D((2,)), hs=D((4, SL)), hv=D((4, SL)), ss=D((2,)), sr=D((2,)), rs=D((2, 11)), rr=D((2, 11)),
        )
        res = pl.pallas_call(
            functools.partial(_kernel, nh, nw, th, tw),
            out_shape=(img, img, wsh, wsh, vec, vec),
            in_specs=[hbm] * 2 + [vm] * 2,
            out_specs=(vm,) * 6,
            scratch_shapes=list(scratch.values()),
            compiler_params=pltpu.CompilerParams(collective_id=0, has_side_effects=True, vmem_limit_bytes=48 << 20),
        )(x.reshape(th, tw, c), g.reshape(th, tw, c), jnp.concatenate([w1, w2]).reshape(2 * NT, c, c),
          jnp.stack([gamma, beta]))
        y, dx, dw1, dw2, dg, db = pl.pallas_call(
            functools.partial(_flush, len(res)),
            out_shape=(img, img, wsp, wsp, vec, vec),
            in_specs=[vm] * len(res),
            out_specs=(hbm,) * len(res),
            scratch_shapes=[D((4 + 2 * NT,))],
            compiler_params=pltpu.CompilerParams(vmem_limit_bytes=1 << 20),
        )(*res)
        return (y.reshape(x.shape), dx.reshape(x.shape), dw1.reshape(3, 3, c, c), dw2.reshape(3, 3, c, c),
                dg.reshape(c), db.reshape(c))

    return jax.shard_map(body, mesh=mesh, in_specs=(tile, P(), P(), P(), P(), tile),
                         out_specs=(tile, tile, P(), P(), P(), P()), check_vma=False)
```

```python
import functools

import jax
import jax.numpy as jnp
from jax import lax
from jax.experimental import pallas as pl
from jax.experimental.pallas import tpu as pltpu
from jax.sharding import PartitionSpec as P

MESH = pl.DeviceIdType.MESH
GROUPS = 32
EPS = 1e-5
RB, TB, NT, SL = 64, 16, 9, 8
C = 128
C2, C3, ZERO = 2 * C, 3 * C, 0.0
BF = jnp.bfloat16
F32 = jnp.float32
GC = 0.7978845608028654
GC2 = GC * 0.044715
DIRS = ((-1, 0), (1, 0), (0, -1), (0, 1), (-1, -1), (-1, 1), (1, -1), (1, 1))
OPP = (1, 0, 3, 2, 7, 6, 5, 4)


def _group_sum(v):
    lane = lax.broadcasted_iota(jnp.int32, v.shape, 1)
    v = v + jnp.where(lane % 2 == 0, pltpu.roll(v, C - 1, 1), pltpu.roll(v, 1, 1))
    return v + jnp.where(lane % 4 < 2, pltpu.roll(v, C - 2, 1), pltpu.roll(v, 2, 1))


def _fold(v):
    return v.reshape(v.shape[0] // SL, SL, C).sum(0)


def _fold_inner(v):
    it = lax.broadcasted_iota(jnp.int32, (SL, C), 0)
    return _fold(v[SL:-SL]) + jnp.where(it == 0, ZERO, v[:SL]) + jnp.where(it == SL - 1, ZERO, v[-SL:])


def _kernel(nh, nw, th, tw, x_hbm, g_hbm, w12, gb,
            y_ref, dx_ref, dw1_ref, dw2_ref, dgam_ref, dbet_ref,
            xv, gv, wc1, wt1, wc2, wt2, ucat, gcat, zcat, gt, dat, av, dn, row,
            hr, hc, hk, hrd, hcd, hkd, ec,
            st, sbuf, tt, tbuf, dwl, rd, rxy, zx_buf,
            ld, hs, hv, ss, sr, rs, rr):
    w = lax.axis_index('w')
    h = lax.axis_index('h')
    ndev = nh * nw
    me = w * nh + h
    w1v, w2v = w12.at[pl.ds(0, NT)], w12.at[pl.ds(NT, NT)]
    cnt = float(th * nh * tw * nw * (C // GROUPS))

    barrier = pltpu.get_barrier_semaphore()

    def others():
        for dw in range(nw - 1, -1, -1):
            for dh in range(nh - 1, -1, -1):
                if dw or dh:
                    yield lax.rem(w + dw, nw), h ^ dh

    for dev in others():
        pl.semaphore_signal(barrier, inc=1, device_id=dev, device_id_type=MESH)

    loads = [pltpu.make_async_copy(s, d, ld.at[i]) for i, (s, d) in enumerate(
        ((x_hbm, xv), (g_hbm, gv)))]
    for c in loads:
        c.start()

    def neighbour(d):
        dy, dx = DIRS[d]
        hh, ww = h + dy, w + dx
        ok = (hh >= 0) & (hh < nh) & (ww >= 0) & (ww < nw)
        return ok, (ww, hh)

    def bufs(t):
        return (hr.at[t], hc.at[t], hk.at[t]) if t < 3 else (hrd, hcd, hkd)

    def halo(t, rows, start):
        cols = ec.at[t]
        hrow, hcol, hcor = bufs(t)
        for d, (dy, dx) in enumerate(DIRS):
            ok, dev = neighbour(d)
            o = OPP[d]
            r = 0 if dy < 0 else rows.shape[0] - 1
            if dx == 0:
                src, dst = rows.at[r], hrow.at[o]
            elif dy == 0:
                src, dst = cols.at[d - 2], hcol.at[o - 2]
            else:
                src, dst = rows.at[r, pl.ds(0 if dx < 0 else tw - TB, TB)], hcor.at[o - 4]
            cp = pltpu.make_async_remote_copy(src, dst, hs.at[t, d], hv.at[t, o], device_id=dev, device_id_type=MESH)
            if start:
                pl.when(ok)(cp.start)
            else:
                back = pltpu.make_async_remote_copy(
                    src, (hrow.at[d] if dx == 0 else hcol.at[d - 2] if dy == 0 else hcor.at[d - 4]),
                    hs.at[t, d], hv.at[t, d], device_id=dev, device_id_type=MESH)

                @pl.when(ok)
                def _():
                    back.wait_send()
                    back.wait_recv()

    okl = [neighbour(d)[0] for d in range(SL)]

    def first(v):
        return v[0]

    def cat_row(cat, r, shifts=(0, 1, 2)):
        for j in range(0, tw, RB):
            for b in shifts:
                cat[r, pl.ds(j, RB), pl.ds(b * C, C)] = row[pl.ds(SL - 1 + b + j, RB), :].astype(BF)

    def shifted(cat):
        @pl.loop(1, th + 1)
        def _(r):
            for j in range(0, tw, RB):
                row[pl.ds(SL + j, RB), :] = cat[r, pl.ds(j, RB), C:C2].astype(F32)
            cat_row(cat, r, (0, 2))

    def set_ends(left, right):
        row[7:SL, :] = left
        row[tw + SL:tw + NT, :] = right

    def patch(cat, r, left, right):
        it = lax.broadcasted_iota(jnp.int32, (TB, C), 0)
        a = cat[r, 0:TB, 0:C].astype(F32)
        cat[r, 0:TB, 0:C] = jnp.where(it == 0, left, a).astype(BF)
        b = cat[r, tw - TB:tw, C2:C3].astype(F32)
        cat[r, tw - TB:tw, C2:C3] = jnp.where(it == 15, right, b).astype(BF)

    def halo_rows(cat, f, *ts):
        hrow, hcol, hcor = zip(*[bufs(t) for t in ts])
        for e, r in ((0, 0), (1, th + 1)):
            for j in range(0, tw, RB):
                row[pl.ds(SL + j, RB), :] = jnp.where(okl[e], f([b[e, pl.ds(j, RB), :].astype(F32) for b in hrow]), ZERO)
            kl, kr = 2 * e, 2 * e + 1
            cl = f([b[kl].astype(F32) for b in hcor])
            cr = f([b[kr].astype(F32) for b in hcor])
            set_ends(jnp.where(okl[4 + kl], cl[15:TB, :], ZERO), jnp.where(okl[4 + kr], cr[0:1, :], ZERO))
            cat_row(cat, r)

        @pl.loop(0, th // SL)
        def _(k):
            r8 = pl.multiple_of(k * SL, SL)
            lf = jnp.where(okl[2], f([b[0, pl.ds(r8, SL), :].astype(F32) for b in hcol]), ZERO)
            rg = jnp.where(okl[3], f([b[1, pl.ds(r8, SL), :].astype(F32) for b in hcol]), ZERO)
            for i in range(SL):
                patch(cat, r8 + i + 1, lf[i:i + 1, :], rg[i:i + 1, :])

    def build(src, cat, t):
        @pl.loop(0, th)
        def _(r):
            for j in range(0, tw, RB):
                row[pl.ds(SL + j, RB), :] = src[r, pl.ds(j, RB), :].astype(F32)
            ec[t, 0, pl.ds(r, 1), :] = row[SL:NT, :]
            ec[t, 1, pl.ds(r, 1), :] = row[tw + SL - 1:tw + SL, :]
            cat_row(cat, r + 1)

    def weights(wv, wc, flip):
        for r in range(4):
            for b in range(3):
                for t in range(2):
                    k = (r - t) * 3 + b
                    ok = t <= r < t + 3
                    v = jnp.zeros((C, C), BF) if not ok else wv[NT - 1 - k].T if flip else wv[k]
                    wc[pl.ds((r * 3 + b) * C, C), pl.ds(t * C, C)] = v

    def dot(blocks, wc):
        lhs = jnp.concatenate([jnp.concatenate(list(b), axis=1) for b in blocks], axis=0)
        return jnp.dot(lhs, wc[...], preferred_element_type=F32)

    def conv(cat, wc, lo, hi, carry, fn):
        for r0 in range(lo, hi, SL):
            n = min(SL, hi - r0)
            o = dot([[cat[r0 + p + r] for r in range(4)] for p in range(0, n, 2)], wc)
            carry = fn(range(r0, r0 + n), o, carry)
        return carry

    def rows_of(o):
        return [o[(i // 2) * tw:(i // 2 + 1) * tw, (i % 2) * C:(i % 2 + 1) * C] for i in range(2 * o.shape[0] // tw)]

    def wgrad_ab(vt, cat, dst):
        for k in (0, 1, th + 2, th + 3):
            vt[k] = jnp.zeros((C, tw), BF)
        lhs = jnp.concatenate([
            jnp.concatenate([vt[i + 2 - a] for a in range(3)], axis=0) for i in range(th + 2)], axis=1)
        rhs = cat[:, :, pl.ds(0, C2)].reshape((th + 2) * tw, C2)
        o = jnp.dot(lhs, rhs, preferred_element_type=F32)
        for b in range(2):
            for a in range(3):
                dst[pl.ds((b * 3 + a) * C, C), :] = o[a * C:(a + 1) * C, b * C:(b + 1) * C].T

    def wgrad_c(vt, cat, dst):
        n = pl.ds(C2, C)
        rows = range(0, th + 2, 2)
        lhs = jnp.concatenate([jnp.concatenate([vt[i + r] for r in range(4)], axis=0) for i in rows], axis=1)
        rhs = jnp.concatenate([jnp.concatenate([cat[i, :, n], cat[i + 1, :, n]], axis=1) for i in rows], axis=0)
        o = jnp.dot(lhs, rhs, preferred_element_type=F32)
        for a in range(3):
            v = [o[(t + 2 - a) * C:(t + 3 - a) * C, t * C:(t + 1) * C] for t in range(2)]
            dst[pl.ds((6 + a) * C, C), :] = (v[0] + v[1]).T

    def spread(src, buf, i):
        buf[me] = src[...]
        for dev in others():
            pltpu.make_async_remote_copy(src, buf.at[me], ss.at[i], sr.at[i], device_id=dev, device_id_type=MESH).start()

    def gather(buf, i):
        part = buf.at[pl.ds(0, ndev - 1)]
        pltpu.make_async_copy(part, part, sr.at[i]).wait()
        pltpu.make_async_copy(part, part, ss.at[i]).wait()
        s = buf[0]
        for k in range(1, ndev):
            s = s + buf[k]
        return s

    core, q_me = h % 2, h // 2
    jobs = ((0, 0, NT * C), (1, 0, NT * C))
    outs = (dw1_ref, dw2_ref)

    def ar_step(i, n):
        k_arr, base, rows = jobs[i]
        src, out = dwl.at[k_arr], outs[k_arr]
        half, piece = rows // 2, rows // 8
        buf = pl.ds(0, piece)

        def sl(c, q=0, n=piece):
            return pl.ds(pl.multiple_of(base + c * half + q * piece, SL), n)

        def cp(a, b, k, dev):
            return pltpu.make_async_remote_copy(a, b, rs.at[i, k], rr.at[i, k], device_id=dev, device_id_type=MESH)

        peer = (w, h ^ 1)
        xy = [(k, (w, h ^ (2 * k))) for k in (3, 2, 1)]
        zp = [(k, lax.rem(w + k, nw), lax.rem(w + nw - k, nw)) for k in range(1, nw)]
        mine = sl(core, q_me)
        pair_rs = cp(src.at[sl(1 - core, 0, half)], rd.at[i, pl.ds(0, half)], 0, peer)
        xy_rs = [cp(src.at[sl(core, q_me ^ k)], rxy.at[i, k - 1, buf], k, dev) for k, dev in xy]
        zx = zx_buf.at[i]
        zx_out = [cp(zx.at[w, buf], zx.at[w, buf], 3 + k, (to, h)) for k, to, _ in zp]
        zx_in = [cp(zx.at[w, buf], zx.at[fr, buf], 3 + k, peer) for k, _, fr in zp]
        xy_out = [cp(out.at[mine], out.at[mine], 6 + k, dev) for k, dev in xy]
        xy_in = [cp(out.at[mine], out.at[sl(core, q_me ^ k)], 6 + k, peer) for k, _ in xy]
        own = out.at[sl(core, 0, half)]
        pair_out = cp(own, own, 10, peer)
        pair_in = cp(own, out.at[sl(1 - core, 0, half)], 10, peer)

        def begin(cps):
            for c in cps:
                c.start()

        def end(sent, got):
            for c in sent:
                c.wait_send()
            for c in got:
                c.wait_recv()

        if n == 0:
            begin([pair_rs])
        elif n == 1:
            end([pair_rs], [pair_rs])
            for k in range(4):
                src[sl(core, k), :] = src[sl(core, k), :] + rd[i, pl.ds(k * piece, piece), :]
            begin(xy_rs)
        elif n == 2:
            end(xy_rs, xy_rs)
            zx[w, buf] = src[mine, :] + rxy[i, 0, buf] + rxy[i, 1, buf] + rxy[i, 2, buf]
            begin(zx_out)
        elif n == 3:
            end(zx_out, zx_in)
            v = zx[0, buf]
            for k in range(1, nw):
                v = v + zx[k, buf]
            out[mine, :] = v
            begin(xy_out)
        elif n == 4:
            end(xy_out, xy_in)
            begin([pair_out])
        else:
            end([pair_out], [pair_in])

    z8 = jnp.zeros((SL, C), F32)
    set_ends(z8[0:1], z8[0:1])
    weights(w1v, wc1, False)
    loads[0].wait()
    build(xv, ucat, 0)

    def fin_a(rows, o, carry):
        s1, s2 = carry
        for r, v in zip(rows, rows_of(o)):
            vb = v.astype(BF)
            av[r] = vb
            vf = vb.astype(F32)
            s1 = s1 + _fold_inner(vf)
            s2 = s2 + _fold_inner(vf * vf)
        return s1, s2

    sums = conv(ucat, wc1, 2, th // 2 + 2, (z8, z8), fin_a)
    pl.semaphore_wait(barrier, ndev - 1)
    halo(0, xv, True)
    sums = conv(ucat, wc1, th // 2 + 2, th - 2, sums, fin_a)

    weights(w2v, wt2, True)
    loads[1].wait()
    build(gv, gcat, 1)
    halo(1, gv, True)

    halo(0, xv, False)
    halo_rows(ucat, first, 0)
    o = dot([[ucat[p + r] for r in range(4)] for p in (0, th - 2)], wc1)
    s1, s2 = fin_a((0, 1, th - 2, th - 1), o, sums)
    it = lax.broadcasted_iota(jnp.int32, (TB, C), 0)
    sides = (pl.ds(0, TB), pl.ds(tw - TB, TB))
    o = dot([[ucat[p + r, s] for r in range(4)] for p in range(0, th, 2) for s in sides], wc1)
    for p in range(th):
        for e, s in enumerate(sides):
            k = (p // 2) * 2 + e
            vb = o[k * TB:(k + 1) * TB, (p % 2) * C:(p % 2 + 1) * C].astype(BF)
            av[p, s] = vb
            vf = jnp.where(it == e * (TB - 1), vb.astype(F32), ZERO)
            ec[2, e, p:p + 1, :] = vf[e * (TB - 1):e * (TB - 1) + 1, :]
            s1 = s1 + _fold(vf)
            s2 = s2 + _fold(vf * vf)
    st[0:1, :] = s1.sum(0, keepdims=True)
    st[1:2, :] = s2.sum(0, keepdims=True)
    spread(st, sbuf, 0)
    halo(2, av, True)

    @pl.loop(0, th)
    def _(r):
        gt[r + 2] = gv[r].T

    halo(1, gv, False)
    halo_rows(gcat, first, 1)

    def fin_dz(rows, o, carry):
        for r, v in zip(rows, rows_of(o)):
            dn[r] = v
        return carry

    conv(gcat, wt2, 0, th, 0, fin_dz)

    tot = _group_sum(gather(sbuf, 0)) / cnt
    mean = tot[0:1, :]
    rstd = lax.rsqrt(tot[1:2, :] - mean * mean + EPS)
    sh = -mean * rstd
    gam, bet = gb[0:1, :], gb[1:2, :]

    def act(a):
        xh = a * rstd + sh
        n = xh * gam + bet
        n2 = n * n
        p = 0.5 + 0.5 * jnp.tanh(n * (GC + GC2 * n2))
        return xh, n2, p, n * p

    def zrow(r, carry):
        t0, t1 = carry
        for j in range(0, tw, RB):
            s = pl.ds(j, RB)
            xh, n2, p, z = act(av[r, s, :].astype(F32))
            zcat[r + 1, s, C:C2] = z.astype(BF)
            d = dn[r, s, :] * (p + z * (1.0 - p) * (2.0 * GC + 6.0 * GC2 * n2))
            dn[r, s, :] = d
            if j == 0:
                ec[3, 0, pl.ds(r, 1), :] = d[0:1, :]
            if j + RB == tw:
                ec[3, 1, pl.ds(r, 1), :] = d[RB - 1:RB, :]
            t0 = t0 + _fold(d * xh)
            t1 = t1 + _fold(d)
        return t0, t1

    t0, t1 = lax.fori_loop(0, th, zrow, (z8, z8))
    tt[0:1, :] = t0.sum(0, keepdims=True)
    tt[1:2, :] = t1.sum(0, keepdims=True)
    spread(tt, tbuf, 1)
    halo(3, dn, True)

    shifted(zcat)
    halo(2, av, False)
    halo_rows(zcat, lambda v: act(v[0])[3], 2)
    wgrad_ab(gt, zcat, dwl.at[1])
    wgrad_c(gt, zcat, dwl.at[1])
    ar_step(1, 0)

    t = gather(tbuf, 1)
    dgam_ref[...] = t[0:1, :]
    dbet_ref[...] = t[1:2, :]
    u = _group_sum(t * gam) / cnt
    k1 = gam * rstd
    k2 = -rstd * rstd * u[0:1, :]
    k3 = -rstd * (u[1:2, :] + sh * u[0:1, :])

    def da_rows(lo, hi):
        @pl.loop(lo, hi)
        def _(r):
            for j in range(0, tw, RB):
                s = pl.ds(j, RB)
                v = (dn[r, s, :] * k1 + av[r, s, :].astype(F32) * k2 + k3).astype(BF)
                gcat[r + 1, s, C:C2] = v
            dat[r + 2] = gcat[r + 1, :, C:C2].T

    da_rows(0, th // 2)
    ar_step(1, 1)
    da_rows(th // 2, th)

    wgrad_ab(dat, ucat, dwl.at[0])
    wgrad_c(dat, ucat, dwl.at[0])
    ar_step(0, 0)
    weights(w1v, wt1, True)
    ar_step(0, 1)
    ar_step(1, 2)

    shifted(gcat)
    halo(3, dn, False)
    halo_rows(gcat, lambda v: v[0] * k1 + v[1] * k2 + k3, 3, 2)

    def fin_dx(rows, o, carry):
        for r, v in zip(rows, rows_of(o)):
            dx_ref[r] = (v + gv[r].astype(F32)).astype(BF)
        return carry

    def fin_y(rows, o, carry):
        for r, v in zip(rows, rows_of(o)):
            y_ref[r] = (v + xv[r].astype(F32)).astype(BF)
        return carry

    conv(gcat, wt1, 0, th, 0, fin_dx)
    weights(w2v, wc2, False)
    ar_step(0, 2)
    ar_step(1, 3)
    conv(zcat, wc2, 0, th, 0, fin_y)
    for i, n in ((1, 4), (0, 3), (1, 5), (0, 4), (0, 5)):
        ar_step(i, n)


def _flush(n, *refs):
    ins, res, sem = refs[:n], refs[n:2 * n], refs[-1]
    cps = []
    for i in range(n):
        if res[i].shape == ins[i].shape:
            cps.append((ins[i], res[i]))
        else:
            cps += [(ins[i].at[pl.ds((k % 3 * 3 + k // 3) * C, C)], res[i].at[k]) for k in range(NT)]
    cps = [pltpu.make_async_copy(a, b, sem.at[k]) for k, (a, b) in enumerate(cps)]
    for c in cps:
        c.start()
    for c in cps:
        c.wait()


def solution(mesh):
    nh, nw = mesh.shape['h'], mesh.shape['w']
    tile = P(None, 'h', 'w', None)

    def body(x, w1, gamma, beta, w2, g):
        _, th, tw, c = x.shape
        hbm = pl.BlockSpec(memory_space=pltpu.HBM)
        vm = pl.BlockSpec(memory_space=pltpu.VMEM)
        V = pltpu.VMEM
        D = pltpu.SemaphoreType.DMA
        img = jax.ShapeDtypeStruct((th, tw, c), BF)
        wsh = jax.ShapeDtypeStruct((NT * c, c), F32)
        wsp = jax.ShapeDtypeStruct((NT, c, c), F32)
        vec = jax.ShapeDtypeStruct((1, c), F32)
        cat = V((th + 2, tw, 3 * c), BF)
        ndev = nh * nw
        scratch = dict(
            xv=V((th, tw, c), BF), gv=V((th, tw, c), BF),
            wc1=V((12 * c, 2 * c), BF), wt1=V((12 * c, 2 * c), BF), wc2=V((12 * c, 2 * c), BF), wt2=V((12 * c, 2 * c), BF),
            ucat=cat, gcat=cat, zcat=cat, gt=V((th + 4, c, tw), BF), dat=V((th + 4, c, tw), BF),
            av=V((th, tw, c), BF), dn=V((th, tw, c), F32), row=V((tw + TB, c), F32),
            hr=V((3, 2, tw, c), BF), hc=V((3, 2, th, c), F32), hk=V((3, 4, TB, c), BF),
            hrd=V((2, tw, c), F32), hcd=V((2, th, c), F32), hkd=V((4, TB, c), F32), ec=V((4, 2, th, c), F32),
            st=V((2, c), F32), sbuf=V((ndev, 2, c), F32), tt=V((2, c), F32), tbuf=V((ndev, 2, c), F32),
            dwl=V((2, NT * c, c), F32),
            rd=V((2, NT * c // 2, c), F32), rxy=V((2, 3, NT * c // SL, c), F32), zx_buf=V((2, nw, NT * c // SL, c), F32),
            ld=D((2,)), hs=D((4, SL)), hv=D((4, SL)), ss=D((2,)), sr=D((2,)), rs=D((2, 11)), rr=D((2, 11)),
        )
        res = pl.pallas_call(
            functools.partial(_kernel, nh, nw, th, tw),
            out_shape=(img, img, wsh, wsh, vec, vec),
            in_specs=[hbm] * 2 + [vm] * 2,
            out_specs=(vm,) * 6,
            scratch_shapes=list(scratch.values()),
            compiler_params=pltpu.CompilerParams(collective_id=0, has_side_effects=True, vmem_limit_bytes=48 << 20),
        )(x.reshape(th, tw, c), g.reshape(th, tw, c), jnp.concatenate([w1, w2]).reshape(2 * NT, c, c),
          jnp.stack([gamma, beta]))
        y, dx, dw1, dw2, dg, db = pl.pallas_call(
            functools.partial(_flush, len(res)),
            out_shape=(img, img, wsp, wsp, vec, vec),
            in_specs=[vm] * len(res),
            out_specs=(hbm,) * len(res),
            scratch_shapes=[D((4 + 2 * NT,))],
            compiler_params=pltpu.CompilerParams(vmem_limit_bytes=1 << 20),
        )(*res)
        return (y.reshape(x.shape), dx.reshape(x.shape), dw1.reshape(3, 3, c, c), dw2.reshape(3, 3, c, c),
                dg.reshape(c), db.reshape(c))

    return jax.shard_map(body, mesh=mesh, in_specs=(tile, P(), P(), P(), P(), tile),
                         out_specs=(tile, tile, P(), P(), P(), P()), check_vma=False)
```
